32 devices in a mesh: gx: 2 (over y), gy: 16 (over z, x, core).
Axes of the slice: x: 2, y: 2, z: 4, core: 2. Of those that a mesh axis runs over, the one named last changes fastest.
Arguments:
- basis_mats: float32 [12, 275, 275], replicated, may hold values from -8 to 8.5, as said below
- coeffs: float32 [512, 12], P(('gx', 'gy')), may hold values from 0.5 to 2
- element_loads: float32 [512, 275], P(('gx', 'gy')), may hold values from -18 to 18
- elem_faces: int32 [512, 6], P(('gx', 'gy')), may hold values from 0 to 71, as said below
- orient_codes: int32 [512, 6], P(('gx', 'gy')), may hold values from 0 to 7
- shared_owned: int32 [32, 2, 4], P(('gx', 'gy')), may hold values from 0 to 63, as said below
- shared_remote: int32 [32, 2, 4], P(('gx', 'gy')), may hold values from 0 to 7, as said below
- lower_peers: int32 [32, 2], P(('gx', 'gy')), may hold values from 0 to 31, as said below
- upper_peers: int32 [32, 2], P(('gx', 'gy')), may hold values from 0 to 31, as said below
Outputs:
- trace: float32 [25, 2048], P(None, ('gx', 'gy'))
- residual: float32 [25, 2048], P(None, ('gx', 'gy'))
The draws below stay inside these ranges and needn't reach their ends.
Inputs may be any that keep to these rules, and one draw needn't show every extreme that they name: `basis_mats`: each matrix is symmetric with every eigenvalue at least 0.5. `elem_faces`: an entry below 64 is a face slot that the element's device owns; an entry 64 + r is that device's remote slot r. Every owned slot of a device is named by one or two of its element faces, every remote slot by exactly one. `shared_owned`: row (d, i) lists 4 distinct owned slots of device d, in message order, that device lower_peers[d, i] uses; the two rows of a device are disjoint. `shared_remote`: row (d, i) lists remote slots of device d in message order: its k-th entry is the face that device upper_peers[d, i] lists k-th in its row i of shared_owned. The two rows of a device together hold each of its 8 remote slots once. upper_peers[lower_peers[d, i], i] = d for every device d and i; the two entries of a row differ. Peers are arbitrary device numbers. lower_peers[upper_peers[d, i], i] = d for every device d and i; the two entries of a row differ; each column is a permutation of the devices. Peers are arbitrary device numbers.
All inputs are finite; a program needn't handle non-finite values.
Results may differ from the reference program's by a relative error of at most 0.0003.
Values sent between devices are 32-bit elements; how exact they have to be, the bound alone decides.
A program may use at most 128 MiB of HBM per device.

```python
import math
import jax
import jax.numpy as jnp
import numpy as np
from jax import lax

SIDE = 5
FACE_DOFS = 25
CELL_DOFS = 125
TRACE_DOFS = 150
LOCAL_DOFS = 275
TERMS = 12
EX = 4
EY = 4
EZ = 1
ITERS = 4
ELEM_DEV = 16
FACE_DEV = 64
SHARED = 4
REMOTE = 8
ELEMS = 512
N_GX = 2
N_GY = 16


def canonical_faces():
    cells = EX * EY * EZ
    plane = EX * EY * EZ
    layout_table = np.zeros((cells, 6), np.int32)
    for first_axis in range(EX):
        for second_axis in range(EY):
            for third_axis in range(EZ):
                cell_index = (first_axis * EY + second_axis) * EZ + third_axis
                layout_table[cell_index, 0] = (first_axis * EY + second_axis) * EZ + third_axis
                if first_axis + 1 < EX:
                    layout_table[cell_index, 1] = ((first_axis + 1) * EY + second_axis) * EZ + third_axis
                else:
                    layout_table[cell_index, 1] = FACE_DEV + second_axis * EZ + third_axis
                layout_table[cell_index, 2] = plane + (second_axis * EX + first_axis) * EZ + third_axis
                if second_axis + 1 < EY:
                    layout_table[cell_index, 3] = plane + ((second_axis + 1) * EX + first_axis) * EZ + third_axis
                else:
                    layout_table[cell_index, 3] = FACE_DEV + SHARED + first_axis * EZ + third_axis
                layout_table[cell_index, 4] = 2 * plane + (third_axis * EX + first_axis) * EY + second_axis
                layout_table[cell_index, 5] = 2 * plane + ((third_axis + 1) * EX + first_axis) * EY + second_axis
    return layout_table


def per_device_orders(key, devices, length):
    sub_keys = jax.random.split(key, devices)
    return jax.vmap(lambda sub_key: jax.random.permutation(sub_key, length))(sub_keys).astype(jnp.int32)


def layout(key):
    devices = N_GX * N_GY
    cells = EX * EY * EZ
    placed = jax.random.permutation(jax.random.fold_in(key, 101), devices).astype(jnp.int32)
    blocks = jnp.argsort(placed).astype(jnp.int32)
    block_row = blocks // N_GY
    block_col = blocks % N_GY
    lower = jnp.stack([placed[(block_row - 1) % N_GX * N_GY + block_col], placed[block_row * N_GY + (block_col - 1) % N_GY]], axis=1)
    upper = jnp.stack([placed[(block_row + 1) % N_GX * N_GY + block_col], placed[block_row * N_GY + (block_col + 1) % N_GY]], axis=1)
    cell_order = per_device_orders(jax.random.fold_in(key, 102), devices, cells)
    owned_order = per_device_orders(jax.random.fold_in(key, 103), devices, FACE_DEV)
    remote_order = per_device_orders(jax.random.fold_in(key, 104), devices, REMOTE)
    canon = jnp.asarray(canonical_faces())
    owned_pick = owned_order[:, jnp.minimum(canon, FACE_DEV - 1)]
    remote_pick = remote_order[:, jnp.clip(canon - FACE_DEV, 0, REMOTE - 1)]
    slots = jnp.where(canon[None] < FACE_DEV, owned_pick, FACE_DEV + remote_pick)
    inverse = jnp.argsort(cell_order, axis=1).astype(jnp.int32)
    stored = jnp.take_along_axis(slots, inverse[:, :, None], axis=1)
    plane = EX * EY * EZ
    owned_lists = jnp.stack([owned_order[:, :SHARED], owned_order[:, plane:plane + SHARED]], axis=1)
    remote_lists = remote_order.reshape(devices, 2, SHARED)
    return (stored.reshape(devices * cells, 6).astype(jnp.int32), owned_lists, remote_lists, lower.astype(jnp.int32), upper.astype(jnp.int32))


def draw_basis_mats(key, part):
    entries = jnp.clip(jax.random.normal(key, (TERMS, LOCAL_DOFS, LOCAL_DOFS), jnp.float32), -4.0, 4.0)
    gram_part = jnp.einsum('kab,kcb->kac', entries, entries, precision=lax.Precision.HIGHEST) / (2.0 * LOCAL_DOFS)
    return gram_part + 0.5 * jnp.eye(LOCAL_DOFS, dtype=jnp.float32)[None]


def draw_elem_faces(key, part):
    return layout(key)[0]


def draw_shared_owned(key, part):
    return layout(key)[1]


def draw_shared_remote(key, part):
    return layout(key)[2]


def draw_lower_peers(key, part):
    return layout(key)[3]


def draw_upper_peers(key, part):
    return layout(key)[4]


def set_ends(array, key, least, largest):
    place = [jax.random.randint(jax.random.fold_in(key, axis), (), 0, length) for axis, length in enumerate(array.shape)]
    main_axis = array.shape.index(max(array.shape))
    next_to = place[:main_axis] + [(place[main_axis] + 1) % array.shape[main_axis]] + place[main_axis + 1:]
    return array.at[tuple(place)].set(least).at[tuple(next_to)].set(largest)


def steps_of(stream_key, shape, cuts, smallest, top_value):
    def one(axis_at, blocks):
        steps = jax.random.uniform(jax.random.fold_in(jax.random.fold_in(stream_key, 6), axis_at), (blocks,), jnp.float32, smallest / len(cuts), top_value / len(cuts))
        return jnp.repeat(jnp.exp(steps), shape[axis_at] // blocks).reshape((-1,) + (1,) * (len(shape) - axis_at - 1))

    gain = one(*cuts[0])
    for cut in cuts[1:]:
        gain = gain * one(*cut)
    return gain


def bell_draw(own_key, dims, deviation, limit, shards=(), held_as=jnp.bfloat16):
    drawn = jax.random.normal(own_key, dims, jnp.float32) * deviation
    if len(shards) > 0:
        drawn = steps_of(own_key, dims, shards, -0.22, 0.18) * drawn
    return jnp.clip(drawn, min=-limit, max=limit).astype(held_as)


def setup_inputs(seed: int = 0) -> dict:
    arg_keys = jax.random.split(jax.random.key(seed), 10)
    return {
        "basis_mats": draw_basis_mats(jax.random.fold_in(arg_keys[9], 71), 0),
        "coeffs": jnp.clip(jnp.exp(math.log(2.0) - 1.3862944 * jax.random.uniform(arg_keys[1], (ELEMS, TERMS), jnp.float32) ** steps_of(arg_keys[1], (ELEMS, TERMS), ((0, 32),), -0.2, 0.2)), 0.5, 2.0),
        "element_loads": bell_draw(arg_keys[2], (ELEMS, LOCAL_DOFS), 3.0, 18.0, ((0, 32),), jnp.float32),
        "elem_faces": draw_elem_faces(jax.random.fold_in(arg_keys[9], 71), 0),
        "orient_codes": set_ends(jax.random.randint(arg_keys[4], (ELEMS, 6), 0, 8), jax.random.fold_in(arg_keys[4], 1), 0, 7).astype(jnp.int32),
        "shared_owned": draw_shared_owned(jax.random.fold_in(arg_keys[9], 71), 0),
        "shared_remote": draw_shared_remote(jax.random.fold_in(arg_keys[9], 71), 0),
        "lower_peers": draw_lower_peers(jax.random.fold_in(arg_keys[9], 71), 0),
        "upper_peers": draw_upper_peers(jax.random.fold_in(arg_keys[9], 71), 0),
    }


full_precision = lax.Precision.HIGHEST

def orient_table():
    edge_nodes = SIDE
    codes_table = np.zeros((8, edge_nodes * edge_nodes), np.int32)
    for code_index in range(8):
        for first_axis in range(edge_nodes):
            for second_axis in range(edge_nodes):
                if code_index & 1:
                    first_new, second_new = (second_axis, first_axis)
                else:
                    first_new, second_new = (first_axis, second_axis)
                if code_index & 2:
                    first_new = edge_nodes - 1 - first_new
                if code_index & 4:
                    second_new = edge_nodes - 1 - second_new
                codes_table[code_index, first_axis * edge_nodes + second_axis] = first_new * edge_nodes + second_new
    return codes_table

def condense(coeffs, element_loads, basis_mats):
    element_mats = jnp.einsum('ek,kab->eab', coeffs, basis_mats, precision=full_precision)
    inner_block = element_mats[:, :CELL_DOFS, :CELL_DOFS]
    coupling = element_mats[:, :CELL_DOFS, CELL_DOFS:]
    outer_block = element_mats[:, CELL_DOFS:, CELL_DOFS:]
    factor = jnp.linalg.cholesky(inner_block)
    solved = jax.scipy.linalg.solve_triangular(factor, coupling, lower=True)
    source = jax.scipy.linalg.solve_triangular(factor, element_loads[:, :CELL_DOFS, None], lower=True)[:, :, 0]
    schur_part = outer_block - jnp.einsum('eib,eic->ebc', solved, solved, precision=full_precision)
    load_trace = element_loads[:, CELL_DOFS:] - jnp.einsum('eib,ei->eb', solved, source, precision=full_precision)
    return (schur_part, load_trace)

def reference(basis_mats, coeffs, element_loads, elem_faces, orient_codes, shared_owned, shared_remote, lower_peers, upper_peers):
    devices = N_GX * N_GY
    elem_total = devices * ELEM_DEV
    face_total = devices * FACE_DEV
    grouped = (coeffs.reshape(devices, ELEM_DEV, TERMS), element_loads.reshape(devices, ELEM_DEV, LOCAL_DOFS))
    schur_blocks, load_trace = lax.map(lambda pieces: condense(pieces[0], pieces[1], basis_mats), grouped)
    schur_blocks = schur_blocks.reshape(elem_total, TRACE_DOFS, TRACE_DOFS)
    load_trace = load_trace.reshape(elem_total, TRACE_DOFS)
    device_ids = jnp.arange(devices, dtype=jnp.int32)
    first_owner = upper_peers[:, 0]
    first_targets = first_owner[:, None] * FACE_DEV + shared_owned[first_owner, 0, :]
    remote_map = jnp.zeros((devices, REMOTE), jnp.int32).at[device_ids[:, None], shared_remote[:, 0, :]].set(first_targets)
    second_users = lower_peers[:, 1]
    second_targets = device_ids[:, None] * FACE_DEV + shared_owned[:, 1, :]
    remote_map = remote_map.at[second_users[:, None], shared_remote[second_users, 1, :]].set(second_targets)
    slot_values = elem_faces.reshape(devices, ELEM_DEV * 6)
    remote_pick = jnp.take_along_axis(remote_map, jnp.clip(slot_values - FACE_DEV, 0, REMOTE - 1).astype(jnp.int32), axis=1)
    face_of = jnp.where(slot_values < FACE_DEV, device_ids[:, None] * FACE_DEV + slot_values, remote_pick).reshape(elem_total, 6)
    codes_table = orient_table()
    forward_idx = jnp.asarray(codes_table)[orient_codes]
    backward_idx = jnp.asarray(np.argsort(codes_table, axis=1).astype(np.int32))[orient_codes]

    def spread(field_values):
        gathered = field_values.T[face_of]
        return jnp.take_along_axis(gathered, forward_idx, axis=2).reshape(elem_total, TRACE_DOFS)

    def collect(element_values):
        placed = jnp.take_along_axis(element_values.reshape(elem_total, 6, FACE_DOFS), backward_idx, axis=2)
        summed = jax.ops.segment_sum(placed.reshape(elem_total * 6, FACE_DOFS), face_of.reshape(-1), num_segments=face_total)
        return summed.T

    def operate(field_values):
        return collect(jnp.einsum('ekl,el->ek', schur_blocks, spread(field_values), precision=full_precision))
    rhs_faces = collect(load_trace)
    diag_faces = collect(jnp.diagonal(schur_blocks, axis1=1, axis2=2))
    trace = jnp.zeros_like(rhs_faces)
    residual = rhs_faces
    precond = residual / diag_faces
    direction = precond
    rz_now = jnp.sum(residual * precond)
    for iteration in range(ITERS):
        mapped = operate(direction)
        step_size = rz_now / jnp.sum(direction * mapped)
        trace = trace + step_size * direction
        residual = residual - step_size * mapped
        precond = residual / diag_faces
        rz_next = jnp.sum(residual * precond)
        direction = precond + rz_next / rz_now * direction
        rz_now = rz_next
    return (trace, residual)
```

```python
import functools

import jax
import jax.numpy as jnp
import numpy as np
from jax import lax
from jax.experimental import pallas as pl
from jax.experimental.pallas import tpu as pltpu
from jax.sharding import PartitionSpec as P

SIDE = 5
FACE_DOFS = 25
CELL_DOFS = 125
TRACE_DOFS = 150
LOCAL_DOFS = 275
ITERS = 4
FACE_DEV = 64
SHARED = 4
REMOTE = 8
LANES = 128
ROWS = 160
NB = 32
BF = jnp.bfloat16
F32 = jnp.float32


def orient_table():
    n = SIDE
    table = np.zeros((8, n * n), np.int32)
    for code in range(8):
        for a in range(n):
            for b in range(n):
                a2, b2 = (b, a) if code & 1 else (a, b)
                if code & 2:
                    a2 = n - 1 - a2
                if code & 4:
                    b2 = n - 1 - b2
                table[code, a * n + b] = a2 * n + b2
    return table


def permute_stack():
    table = orient_table()
    out = np.zeros((32, 256), np.float32)
    for code in range(8):
        for q in range(FACE_DOFS):
            out[q, 32 * code + table[code, q]] = 1.0
    return out


def iota(shape, dim):
    return lax.broadcasted_iota(jnp.int32, shape, dim)


def hi_part(x):
    return x.astype(BF).astype(F32)


def pack_lanes(x, source):
    lane = iota(x.shape, 1)

    def at(place):
        shift = (place - source) % LANES
        return x if shift == 0 else pltpu.roll(x, shift, 1)

    x0, x1, x2 = at(0), at(NB), at(2 * NB)
    packed = jnp.where(lane < NB, x0, jnp.where(lane < 2 * NB, x1 - hi_part(x1), x2))
    return jnp.where(lane < 3 * NB, packed, 0.0).astype(BF)


def pack_rows(x):
    high = x.astype(BF)
    low = (x - high.astype(F32)).astype(BF)
    return jnp.concatenate([high, high, low, jnp.zeros_like(high)], axis=0)


def invert_blocks(tiles):
    lane = iota((8, LANES), 1)
    sub = iota((8, LANES), 0)
    inside = lane % NB
    first = lane - inside
    for k in range(NB):
        tk, sk = k // 8, k % 8
        pick = first + k
        here = inside == k
        for g in range(len(tiles)):
            group = tiles[g]
            row = jnp.broadcast_to(group[tk][sk : sk + 1, :], (8, LANES))
            pivot = jnp.take_along_axis(row, pick, axis=1)
            inverse = 1.0 / pivot
            new_row = jnp.where(here, inverse, row * inverse)
            fresh = []
            for t in range(4):
                column = jnp.take_along_axis(group[t], pick, axis=1)
                value = jnp.where(here, 0.0, group[t]) - column * new_row
                if t == tk:
                    value = jnp.where(sub == sk, new_row, value)
                fresh.append(value)
            tiles[g] = fresh
    return tiles


def condense_kernel(elems, terms, coef_ref, basis_ref, load_ref, shi_ref, slo_ref, diag_ref, lrow_ref, x_ref, d_ref):
    lane8 = iota((8, LANES), 1)
    sub8 = iota((8, LANES), 0)
    tail = LOCAL_DOFS - 256

    def combine(row_slice, count, emit):
        parts = [
            [basis_ref[k, row_slice, 0:128], basis_ref[k, row_slice, 128:256], basis_ref[k, row_slice, 256:LOCAL_DOFS]]
            for k in range(terms)
        ]
        for e in range(elems):
            total = None
            for k in range(terms):
                scaled = [coef_ref[e, k] * part for part in parts[k]]
                total = scaled if total is None else [a + b for a, b in zip(total, scaled)]
            t0, t1, t2 = total
            t2 = jnp.concatenate([t2, jnp.zeros((count, LANES - tail), F32)], axis=1)
            if count < 8:
                t0, t1, t2 = (
                    jnp.concatenate([t, jnp.zeros((8 - count, LANES), F32)], axis=0) for t in (t0, t1, t2)
                )
            emit(e, t0, t1, t2)

    def put_inner(e, start, t0, t1, t2, edge):
        inner = lane8 < CELL_DOFS
        moved = jnp.where(inner, t2, t0)
        kept = jnp.where(inner, t0, 0.0)
        if edge:
            good = sub8 + 120 < CELL_DOFS
            kept = jnp.where(good, kept, jnp.where(sub8 + 120 == lane8, 1.0, 0.0))
            t1 = jnp.where(good, t1, 0.0)
            moved = jnp.where(good, moved, 0.0)
        x_ref[e, pl.ds(start, 8), 0:128] = kept
        x_ref[e, pl.ds(start, 8), 128:256] = t1
        x_ref[e, pl.ds(start, 8), 256:384] = moved

    def put_outer(e, start, t0, t1, t2):
        inner = lane8 < CELL_DOFS
        x_ref[e, pl.ds(start, 8), 0:128] = jnp.where(inner, t0, 0.0)
        x_ref[e, pl.ds(start, 8), 128:256] = t1
        x_ref[e, pl.ds(start, 8), 256:384] = jnp.where(inner, t2, t0)

    @pl.loop(0, 15)
    def _(t):
        start = pl.multiple_of(t * 8, 8)
        combine(pl.ds(start, 8), 8, lambda e, a, b, c: put_inner(e, start, a, b, c, False))

    def edge_rows(e, t0, t1, t2):
        put_inner(e, 120, t0, t1, t2, True)
        first = sub8 == 0

        def with_load(tile, lo):
            return jnp.where(first, jnp.broadcast_to(load_ref[e : e + 1, lo : lo + 128], (8, LANES)), tile)

        put_outer(e, 128, with_load(t0, 0), with_load(t1, 128), with_load(t2, 256))

    combine(pl.ds(120, 8), 8, edge_rows)

    @pl.loop(16, 34)
    def _(t):
        start = pl.multiple_of(t * 8, 8)
        combine(pl.ds(start, 8), 8, lambda e, a, b, c: put_outer(e, start + 8, a, b, c))

    combine(pl.ds(272, 3), 3, lambda e, a, b, c: put_outer(e, 280, a, b, c))

    groups = elems // 4
    lane32 = iota((NB, LANES), 1)
    for b in range(4):
        rows = slice(NB * b, NB * b + NB)
        tiles = []
        for g in range(groups):
            whole = jnp.zeros((NB, LANES), F32)
            for q in range(4):
                part = x_ref[g * 4 + q, rows, 0:128]
                shift = (NB * (q - b)) % LANES
                if shift:
                    part = pltpu.roll(part, shift, 1)
                whole = jnp.where(lane32 // NB == q, part, whole)
            tiles.append([whole[8 * t : 8 * t + 8] for t in range(4)])
        tiles = invert_blocks(tiles)
        for g in range(groups):
            whole = jnp.concatenate(tiles[g], axis=0)
            for q in range(4):
                d_ref[g * 4 + q] = pack_lanes(whole, NB * q)
        lo = 0 if b < 3 else LANES

        @pl.loop(0, elems)
        def _(e):
            scaled = jnp.dot(d_ref[e], pack_rows(x_ref[e, rows, lo:384]), preferred_element_type=F32)
            lhs = pack_lanes(x_ref[e, NB * (b + 1) : 288, 0:128], NB * b)
            update = jnp.dot(lhs, pack_rows(scaled), preferred_element_type=F32)
            x_ref[e, NB * (b + 1) : 288, lo:384] = x_ref[e, NB * (b + 1) : 288, lo:384] - update

    diag_ref[...] = jnp.zeros_like(diag_ref)
    lane_w = iota((ROWS, 256), 1)
    on_diag = (iota((ROWS, 256), 0) + 248) % 256 == lane_w
    lane_t = iota((ROWS, LANES), 1)

    @pl.loop(0, elems)
    def _(e):
        s = x_ref[e, 128:288, 128:384]
        high = s.astype(BF)
        start = pl.multiple_of(e * ROWS, 32)
        shi_ref[pl.ds(start, ROWS), :] = high
        slo_ref[pl.ds(start, ROWS), :] = (s - high.astype(F32)).astype(BF)
        only = jnp.where(on_diag, s, 0.0)
        column = jnp.sum(only[:, 0:128] + only[:, 128:256], axis=1, keepdims=True)
        diag_ref[...] = jnp.where(lane_t == e, column, diag_ref[...])
        lrow_ref[pl.ds(e, 1), :] = s[0:1, :]


def split3(x):
    a = x.astype(BF)
    rest = x - a.astype(F32)
    b = rest.astype(BF)
    c = (rest - b.astype(F32)).astype(BF)
    return a, b, c


def cg_kernel(
    mesh_names, sizes, elems, upper_ref, lower_ref, ints_ref, perm_ref, permt_ref, shi_ref, slo_ref, diag_ref, lrow_ref,
    trace_ref, resid_ref, buf_refs, send_ref, send_sem, recv_sem,
):
    devices = sizes[0] * sizes[1]
    me = lax.axis_index(mesh_names[0]) * sizes[1] + lax.axis_index(mesh_names[1])

    def coords(d):
        return (d // sizes[1], lax.rem(d, sizes[1]))

    barrier = pltpu.get_barrier_semaphore()

    def greet(k, carry):
        pl.semaphore_signal(
            barrier, inc=1, device_id=coords(lax.rem(me + k, devices)), device_id_type=pl.DeviceIdType.MESH
        )
        return carry

    lax.fori_loop(1, devices, greet, 0)

    square = (LANES, LANES)
    sub = iota(square, 0)
    inc_t = jnp.where(sub == ints_ref[0:1, :], 1.0, 0.0)
    inc = inc_t.T
    sel = jnp.where(sub == ints_ref[2:3, :], 1.0, 0.0).astype(BF)
    place = jnp.where(sub == ints_ref[3:4, :], 1.0, 0.0).T.astype(BF)
    inc_t = inc_t.astype(BF)
    inc = inc.astype(BF)
    inc_sel = jnp.dot(inc, sel, preferred_element_type=F32).astype(BF)
    out_mat = jnp.concatenate([inc, inc_sel], axis=1)
    perm = perm_ref[...]
    perm_t = permt_ref[...]
    code = ints_ref[1:2, :]
    lane32 = iota((32, LANES), 1)
    sub32 = iota((32, LANES), 0)
    in_group = lane32 // 16 == sub32 // 4
    lane4 = iota((4, LANES), 1)
    slot4 = lane4 % 16
    owned = lane32 < FACE_DEV

    def spread(field):
        a, b, c = split3(field)
        got = jnp.dot(jnp.concatenate([a, b, c], axis=0), inc_t, preferred_element_type=F32)
        pieces = []
        for s in range(3):
            part = got[32 * s : 32 * s + 32]
            pieces.append(
                jnp.concatenate([jnp.where(code == o, part, 0.0) for o in range(8)], axis=0).astype(BF)
            )
        return jnp.dot(perm, jnp.concatenate(pieces, axis=1), preferred_element_type=F32)

    def columns(values):
        blocks = []
        for j in range(6):
            block = jnp.zeros((32, LANES), F32)
            for s in range(3):
                part = values[:, LANES * s : LANES * s + LANES]
                shift = (16 * s - 16 * j) % LANES
                if shift:
                    part = pltpu.roll(part, shift, 1)
                block = jnp.where(lane32 // 16 == s, part, block)
            blocks.append(block)
        return jnp.concatenate(
            [blocks[0][3:25]] + [x[0:25] for x in blocks[1:]] + [jnp.zeros((106, LANES), F32), blocks[0][0:3]], axis=0
        ).astype(BF)

    def by_face(slices):
        out = jnp.zeros((32, LANES), F32)
        for j in range(6):
            part = jnp.concatenate([slices[j], jnp.zeros((7, LANES), F32)], axis=0)
            if j:
                part = pltpu.roll(part, 16 * j, 1)
            out = jnp.where(lane32 // 16 == j, part, out)
        return out

    def from_rows(t):
        return by_face([t[5 + 25 * j : 30 + 25 * j] for j in range(6)])

    def collect(values):
        turned = jnp.dot(perm_t, jnp.concatenate(split3(values), axis=1), preferred_element_type=F32)
        turned = turned[:, 0:128] + turned[:, 128:256] + turned[:, 256:384]
        placed = jnp.zeros((32, LANES), F32)
        for o in range(8):
            placed = jnp.where(code == o, turned[32 * o : 32 * o + 32], placed)
        both = jnp.dot(jnp.concatenate(split3(placed), axis=0), out_mat, preferred_element_type=F32)
        both = both[0:32] + both[32:64] + both[64:96]
        return both[:, 0:128], both[:, 128:256]

    def pack(message):
        kept = jnp.where(in_group, message, 0.0)
        out = kept[0:4]
        for g in range(1, 8):
            out = out + kept[4 * g : 4 * g + 4]
        return out

    def unpack(message):
        tall = jnp.where(in_group, jnp.concatenate([message] * 8, axis=0), 0.0)
        both = jnp.dot(jnp.concatenate(split3(tall), axis=0), place, preferred_element_type=F32)
        return both[0:32] + both[32:64] + both[64:96]

    def exchange(slot, parts):
        count = len(parts)
        buf_ref = buf_refs[slot]
        own_rows = send_ref.at[slot, 0 : 4 * count]
        for i, part in enumerate(parts):
            send_ref[slot, 4 * i : 4 * i + 4] = part
            buf_ref[me, 4 * i : 4 * i + 4] = part

        def send(k, carry):
            pltpu.make_async_remote_copy(
                src_ref=own_rows,
                dst_ref=buf_ref.at[me],
                send_sem=send_sem.at[slot],
                recv_sem=recv_sem.at[slot],
                device_id=coords(lax.rem(me + k, devices)),
                device_id_type=pl.DeviceIdType.MESH,
            ).start()
            return carry

        lax.fori_loop(1, devices, send, 0)
        every = buf_ref.at[pl.ds(0, devices - 1)]
        pltpu.make_async_copy(every, every, recv_sem.at[slot]).wait()
        pltpu.make_async_copy(every, every, send_sem.at[slot]).wait()
        from_upper = [buf_ref[upper_ref[0, i]] for i in range(2)]
        from_lower = [buf_ref[lower_ref[0, i]] for i in range(2)]
        out = []
        for i in range(count):
            rows = slice(4 * i, 4 * i + 4)
            mixed = jnp.where(
                slot4 < 4,
                from_upper[0][rows],
                jnp.where(
                    slot4 < 8, from_upper[1][rows], jnp.where(slot4 < 12, from_lower[0][rows], from_lower[1][rows])
                ),
            )
            out.append(unpack(mixed))
        return out

    spare = (lane4 // 16 == 6) & (iota((4, LANES), 0) == 1)

    diag_part, diag_out = collect(from_rows(diag_ref[...]))
    padded = jnp.concatenate([lrow_ref[...], jnp.zeros((LANES - elems, 256), F32)], axis=0)
    turned = jnp.concatenate([padded[:, 0:128].T, padded[:, 128:256].T], axis=0)
    slices = [jnp.concatenate([turned[253:256], turned[0:22]], axis=0)]
    slices += [turned[25 * j - 3 : 25 * j + 22] for j in range(1, 6)]
    load_part, load_out = collect(by_face(slices))
    pl.semaphore_wait(barrier, devices - 1)
    got = exchange(0, [pack(load_out), pack(diag_out)])
    live = (lane32 < FACE_DEV + REMOTE) & (sub32 < FACE_DOFS)
    residual = jnp.where(live, load_part + got[0], 0.0)
    weights = jnp.where(live, 1.0 / jnp.where(live, diag_part + got[1], 1.0), 0.0)

    trace = jnp.zeros((32, LANES), F32)
    direction = jnp.zeros((32, LANES), F32)
    image = jnp.zeros((32, LANES), F32)
    rz_now = None
    step = None
    row_lane = iota((ROWS, LANES), 1)
    row_elem = jnp.where(row_lane < 48, row_lane % 16, -1)
    for iteration in range(ITERS):
        precond = residual * weights
        values = spread(precond)
        cols = columns(values)
        total = jnp.zeros((ROWS, LANES), F32)
        for e in range(elems):
            rows = slice(ROWS * e, ROWS * e + ROWS)
            product = jnp.dot(shi_ref[rows], cols, preferred_element_type=F32)
            product = product + jnp.dot(slo_ref[rows], cols, preferred_element_type=F32)
            total = jnp.where(row_elem == e, product, total)
        total = total + pltpu.roll(total, LANES - 16, 1) + pltpu.roll(total, LANES - 32, 1)
        result = from_rows(total)
        flat = values[:, 0:128] + values[:, 128:256] + values[:, 256:384]
        curve_part = jnp.sum(jnp.where(lane32 < 6 * elems, flat * result, 0.0))
        rz_part = jnp.sum(jnp.where(owned, residual * precond, 0.0))
        part, out = collect(result)
        message = pack(out)
        message = jnp.where(spare, jnp.where(slot4 == 0, rz_part, jnp.where(slot4 == 1, curve_part, 0.0)), message)
        slot = iteration + 1
        got = exchange(slot, [message])[0]

        def add(d, carry):
            return carry + buf_refs[slot][d]

        sums = lax.fori_loop(0, devices, add, jnp.zeros((4, LANES), F32))
        rz_next = jnp.sum(jnp.where(spare & (slot4 == 0), sums, 0.0), keepdims=True)
        curve = jnp.sum(jnp.where(spare & (slot4 == 1), sums, 0.0), keepdims=True)
        mapped = jnp.where(live, part + got, 0.0)
        if iteration == 0:
            step = rz_next / curve
            direction, image = precond, mapped
        else:
            ratio = rz_next / rz_now
            step = rz_next / (curve - ratio * rz_next / step)
            direction = precond + ratio * direction
            image = mapped + ratio * image
        rz_now = rz_next
        trace = trace + step * direction
        residual = residual - step * image
    trace_ref[...] = trace[0:FACE_DOFS, 0:FACE_DEV]
    resid_ref[...] = residual[0:FACE_DOFS, 0:FACE_DEV]


def on_device(
    sizes, basis_mats, coeffs, element_loads, elem_faces, orient_codes, shared_owned, shared_remote, lower_peers, upper_peers
):
    elems, terms = coeffs.shape
    vmem = pl.BlockSpec(memory_space=pltpu.VMEM)
    smem = pl.BlockSpec(memory_space=pltpu.SMEM)
    loads = jnp.pad(element_loads, ((0, 0), (0, 384 - LOCAL_DOFS)))
    shi, slo, diag, lrow = pl.pallas_call(
        functools.partial(condense_kernel, elems, terms),
        out_shape=(
            jax.ShapeDtypeStruct((elems * ROWS, 256), BF),
            jax.ShapeDtypeStruct((elems * ROWS, 256), BF),
            jax.ShapeDtypeStruct((ROWS, LANES), F32),
            jax.ShapeDtypeStruct((elems, 256), F32),
        ),
        in_specs=[smem, vmem, vmem],
        out_specs=(vmem, vmem, vmem, vmem),
        scratch_shapes=[pltpu.VMEM((elems, 288, 384), F32), pltpu.VMEM((elems, NB, LANES), BF)],
        compiler_params=pltpu.CompilerParams(vmem_limit_bytes=40 * 1024 * 1024),
        name="condense",
    )(coeffs, basis_mats, loads)

    def lane_row(values, fill):
        flat = values.reshape(1, -1)
        return jnp.pad(flat, ((0, 0), (0, LANES - flat.shape[1])), constant_values=fill)

    own = shared_owned.reshape(-1)
    far = FACE_DEV + shared_remote.reshape(-1)
    ints = jnp.concatenate(
        [
            lane_row(elem_faces.T, -1),
            lane_row(orient_codes.T, 0),
            jnp.tile(jnp.concatenate([own, far]), 8)[None],
            jnp.tile(jnp.concatenate([far, own]), 8)[None],
            jnp.zeros((4, LANES), jnp.int32),
        ],
        axis=0,
    )
    stack = permute_stack()
    devices = sizes[0] * sizes[1]
    return pl.pallas_call(
        functools.partial(cg_kernel, ("gx", "gy"), sizes, elems),
        out_shape=(
            jax.ShapeDtypeStruct((FACE_DOFS, FACE_DEV), F32),
            jax.ShapeDtypeStruct((FACE_DOFS, FACE_DEV), F32),
        ),
        in_specs=[smem, smem] + [vmem] * 7,
        out_specs=(vmem, vmem),
        scratch_shapes=[
            [pltpu.VMEM((devices, 8 if i == 0 else 4, LANES), F32) for i in range(ITERS + 1)],
            pltpu.VMEM((ITERS + 1, 8, LANES), F32),
            pltpu.SemaphoreType.DMA((ITERS + 1,)),
            pltpu.SemaphoreType.DMA((ITERS + 1,)),
        ],
        compiler_params=pltpu.CompilerParams(
            collective_id=0, has_side_effects=True, vmem_limit_bytes=48 * 1024 * 1024
        ),
        name="solve",
    )(
        upper_peers, lower_peers, ints, jnp.asarray(stack, BF), jnp.asarray(stack.T, BF), shi, slo, diag, lrow
    )


def solution(mesh):
    row = P(("gx", "gy"), None)
    cube = P(("gx", "gy"), None, None)
    sizes = (mesh.shape["gx"], mesh.shape["gy"])
    return jax.shard_map(
        functools.partial(on_device, sizes),
        mesh=mesh,
        in_specs=(P(), row, row, row, row, cube, cube, row, row),
        out_specs=(P(None, ("gx", "gy")), P(None, ("gx", "gy"))),
        check_vma=False,
    )
```

```python
import functools

import jax
import jax.numpy as jnp
import numpy as np
from jax import lax
from jax.experimental import pallas as pl
from jax.experimental.pallas import tpu as pltpu
from jax.sharding import PartitionSpec as P

SIDE = 5
FACE_DOFS = 25
CELL_DOFS = 125
TRACE_DOFS = 150
LOCAL_DOFS = 275
ITERS = 4
FACE_DEV = 64
SHARED = 4
REMOTE = 8
LANES = 128
ROWS = 160
NB = 32
WAYS = 4
BF = jnp.bfloat16
F32 = jnp.float32


def orient_table():
    n = SIDE
    table = np.zeros((8, n * n), np.int32)
    for code in range(8):
        for a in range(n):
            for b in range(n):
                a2, b2 = (b, a) if code & 1 else (a, b)
                if code & 2:
                    a2 = n - 1 - a2
                if code & 4:
                    b2 = n - 1 - b2
                table[code, a * n + b] = a2 * n + b2
    return table


def permute_stack():
    table = orient_table()
    out = np.zeros((32, 256), np.float32)
    for code in range(8):
        for q in range(FACE_DOFS):
            out[q, 32 * code + table[code, q]] = 1.0
    return out


def iota(shape, dim):
    return lax.broadcasted_iota(jnp.int32, shape, dim)


def hi_part(x):
    return x.astype(BF).astype(F32)


def pack_lanes(x, source):
    lane = iota(x.shape, 1)

    def at(place):
        shift = (place - source) % LANES
        return x if shift == 0 else pltpu.roll(x, shift, 1)

    x0, x1, x2 = at(0), at(NB), at(2 * NB)
    packed = jnp.where(lane < NB, x0, jnp.where(lane < 2 * NB, x1 - hi_part(x1), x2))
    return jnp.where(lane < 3 * NB, packed, 0.0).astype(BF)


def pack_rows(x):
    high = x.astype(BF)
    low = (x - high.astype(F32)).astype(BF)
    return jnp.concatenate([high, high, low, jnp.zeros_like(high)], axis=0)


def invert_blocks(tiles):
    lane = iota((8, LANES), 1)
    sub = iota((8, LANES), 0)
    inside = lane % NB
    first = lane - inside
    for k in range(NB):
        tk, sk = k // 8, k % 8
        pick = first + k
        here = inside == k
        for g in range(len(tiles)):
            group = tiles[g]
            row = jnp.broadcast_to(group[tk][sk : sk + 1, :], (8, LANES))
            pivot = jnp.take_along_axis(row, pick, axis=1)
            inverse = 1.0 / pivot
            new_row = jnp.where(here, inverse, row * inverse)
            fresh = []
            for t in range(4):
                column = jnp.take_along_axis(group[t], pick, axis=1)
                value = jnp.where(here, 0.0, group[t]) - column * new_row
                if t == tk:
                    value = jnp.where(sub == sk, new_row, value)
                fresh.append(value)
            tiles[g] = fresh
    return tiles


def condense_kernel(elems, terms, coef_ref, basis_ref, load_ref, shi_ref, slo_ref, diag_ref, lrow_ref, x_refs, d_ref, r_refs):
    lane8 = iota((8, LANES), 1)
    sub8 = iota((8, LANES), 0)
    tail = LOCAL_DOFS - 256

    def combine(row_slice, count, emit):
        parts = [
            [basis_ref[k, row_slice, 0:128], basis_ref[k, row_slice, 128:256], basis_ref[k, row_slice, 256:LOCAL_DOFS]]
            for k in range(terms)
        ]
        for e in range(elems):
            total = None
            for k in range(terms):
                scaled = [coef_ref[e, k] * part for part in parts[k]]
                total = scaled if total is None else [a + b for a, b in zip(total, scaled)]
            t0, t1, t2 = total
            t2 = jnp.concatenate([t2, jnp.zeros((count, LANES - tail), F32)], axis=1)
            if count < 8:
                t0, t1, t2 = (
                    jnp.concatenate([t, jnp.zeros((8 - count, LANES), F32)], axis=0) for t in (t0, t1, t2)
                )
            emit(e, t0, t1, t2)

    def put(e, start, *tiles):
        for i, tile in enumerate(tiles):
            x_refs[e % WAYS][e // WAYS, pl.ds(start, 8), LANES * i : LANES * i + LANES] = tile

    def put_inner(e, start, t0, t1, t2, edge):
        inner = lane8 < CELL_DOFS
        moved = jnp.where(inner, t2, t0)
        kept = jnp.where(inner, t0, 0.0)
        if edge:
            good = sub8 + 120 < CELL_DOFS
            kept = jnp.where(good, kept, jnp.where(sub8 + 120 == lane8, 1.0, 0.0))
            t1 = jnp.where(good, t1, 0.0)
            moved = jnp.where(good, moved, 0.0)
        put(e, start, kept, t1, moved)

    def put_outer(e, start, t0, t1, t2):
        inner = lane8 < CELL_DOFS
        put(e, start, jnp.where(inner, t0, 0.0), t1, jnp.where(inner, t2, t0))

    @pl.loop(0, 15)
    def _(t):
        start = pl.multiple_of(t * 8, 8)
        combine(pl.ds(start, 8), 8, lambda e, a, b, c: put_inner(e, start, a, b, c, False))

    def edge_rows(e, t0, t1, t2):
        put_inner(e, 120, t0, t1, t2, True)
        first = sub8 == 0

        def with_load(tile, lo):
            return jnp.where(first, jnp.broadcast_to(load_ref[e : e + 1, lo : lo + 128], (8, LANES)), tile)

        put_outer(e, 128, with_load(t0, 0), with_load(t1, 128), with_load(t2, 256))

    combine(pl.ds(120, 8), 8, edge_rows)

    @pl.loop(16, 34)
    def _(t):
        start = pl.multiple_of(t * 8, 8)
        combine(pl.ds(start, 8), 8, lambda e, a, b, c: put_outer(e, start + 8, a, b, c))

    combine(pl.ds(272, 3), 3, lambda e, a, b, c: put_outer(e, 280, a, b, c))

    groups = elems // 4
    lane32 = iota((NB, LANES), 1)
    for b in range(4):
        rows = slice(NB * b, NB * b + NB)
        tiles = []
        for g in range(groups):
            whole = jnp.zeros((NB, LANES), F32)
            for q in range(4):
                part = x_refs[q][g, rows, 0:128]
                shift = (NB * (q - b)) % LANES
                if shift:
                    part = pltpu.roll(part, shift, 1)
                whole = jnp.where(lane32 // NB == q, part, whole)
            tiles.append([whole[8 * t : 8 * t + 8] for t in range(4)])
        tiles = invert_blocks(tiles)
        for g in range(groups):
            whole = jnp.concatenate(tiles[g], axis=0)
            for q in range(4):
                d_ref[g * 4 + q] = pack_lanes(whole, NB * q)
        lo = 0 if b < 3 else LANES

        below = slice(NB * (b + 1), 288)

        @pl.loop(0, groups)
        def _(g):
            for q in range(WAYS):
                scaled = jnp.dot(
                    d_ref[g * WAYS + q], pack_rows(x_refs[q][g, rows, lo:384]), preferred_element_type=F32
                )
                r_refs[q][:, lo:384] = pack_rows(scaled)
            for q in range(WAYS):
                lhs = pack_lanes(x_refs[q][g, below, 0:128], NB * b)
                update = jnp.dot(lhs, r_refs[q][:, lo:384], preferred_element_type=F32)
                x_refs[q][g, below, lo:384] = x_refs[q][g, below, lo:384] - update

    diag_ref[...] = jnp.zeros_like(diag_ref)
    lane_w = iota((ROWS, 256), 1)
    on_diag = (iota((ROWS, 256), 0) + 248) % 256 == lane_w
    lane_t = iota((ROWS, LANES), 1)

    @pl.loop(0, groups)
    def _(g):
        for q in range(WAYS):
            e = g * WAYS + q
            s = x_refs[q][g, 128:288, 128:384]
            high = s.astype(BF)
            start = pl.multiple_of(e * ROWS, 32)
            shi_ref[pl.ds(start, ROWS), :] = high
            slo_ref[pl.ds(start, ROWS), :] = (s - high.astype(F32)).astype(BF)
            only = jnp.where(on_diag, s, 0.0)
            column = jnp.sum(only[:, 0:128] + only[:, 128:256], axis=1, keepdims=True)
            diag_ref[...] = jnp.where(lane_t == e, column, diag_ref[...])
            lrow_ref[pl.ds(e, 1), :] = s[0:1, :]


def split3(x):
    a = x.astype(BF)
    rest = x - a.astype(F32)
    b = rest.astype(BF)
    c = (rest - b.astype(F32)).astype(BF)
    return a, b, c


def cg_kernel(
    mesh_names, sizes, elems, upper_ref, lower_ref, ints_ref, perm_ref, permt_ref, shi_ref, slo_ref, diag_ref, lrow_ref,
    trace_ref, resid_ref, buf_refs, send_ref, send_sem, recv_sem,
):
    devices = sizes[0] * sizes[1]
    me = lax.axis_index(mesh_names[0]) * sizes[1] + lax.axis_index(mesh_names[1])

    def coords(d):
        return (d // sizes[1], lax.rem(d, sizes[1]))

    barrier = pltpu.get_barrier_semaphore()

    def greet(k, carry):
        pl.semaphore_signal(
            barrier, inc=1, device_id=coords(lax.rem(me + k, devices)), device_id_type=pl.DeviceIdType.MESH
        )
        return carry

    lax.fori_loop(1, devices, greet, 0)

    square = (LANES, LANES)
    sub = iota(square, 0)
    inc_t = jnp.where(sub == ints_ref[0:1, :], 1.0, 0.0)
    inc = inc_t.T
    sel = jnp.where(sub == ints_ref[2:3, :], 1.0, 0.0).astype(BF)
    place = jnp.where(sub == ints_ref[3:4, :], 1.0, 0.0).T.astype(BF)
    inc_t = inc_t.astype(BF)
    inc = inc.astype(BF)
    inc_sel = jnp.dot(inc, sel, preferred_element_type=F32).astype(BF)
    out_mat = jnp.concatenate([inc, inc_sel], axis=1)
    perm = perm_ref[...]
    perm_t = permt_ref[...]
    code = ints_ref[1:2, :]
    lane32 = iota((32, LANES), 1)
    sub32 = iota((32, LANES), 0)
    in_group = lane32 // 16 == sub32 // 4
    lane4 = iota((4, LANES), 1)
    slot4 = lane4 % 16
    owned = lane32 < FACE_DEV

    def spread(field):
        a, b, c = split3(field)
        got = jnp.dot(jnp.concatenate([a, b, c], axis=0), inc_t, preferred_element_type=F32)
        pieces = []
        for s in range(3):
            part = got[32 * s : 32 * s + 32]
            pieces.append(
                jnp.concatenate([jnp.where(code == o, part, 0.0) for o in range(8)], axis=0).astype(BF)
            )
        return jnp.dot(perm, jnp.concatenate(pieces, axis=1), preferred_element_type=F32)

    def columns(values):
        blocks = []
        for j in range(6):
            block = jnp.zeros((32, LANES), F32)
            for s in range(3):
                part = values[:, LANES * s : LANES * s + LANES]
                shift = (16 * s - 16 * j) % LANES
                if shift:
                    part = pltpu.roll(part, shift, 1)
                block = jnp.where(lane32 // 16 == s, part, block)
            blocks.append(block)
        return jnp.concatenate(
            [blocks[0][3:25]] + [x[0:25] for x in blocks[1:]] + [jnp.zeros((106, LANES), F32), blocks[0][0:3]], axis=0
        ).astype(BF)

    def by_face(slices):
        out = jnp.zeros((32, LANES), F32)
        for j in range(6):
            part = jnp.concatenate([slices[j], jnp.zeros((7, LANES), F32)], axis=0)
            if j:
                part = pltpu.roll(part, 16 * j, 1)
            out = jnp.where(lane32 // 16 == j, part, out)
        return out

    def from_rows(t):
        return by_face([t[5 + 25 * j : 30 + 25 * j] for j in range(6)])

    def collect(values):
        turned = jnp.dot(perm_t, jnp.concatenate(split3(values), axis=1), preferred_element_type=F32)
        turned = turned[:, 0:128] + turned[:, 128:256] + turned[:, 256:384]
        placed = jnp.zeros((32, LANES), F32)
        for o in range(8):
            placed = jnp.where(code == o, turned[32 * o : 32 * o + 32], placed)
        both = jnp.dot(jnp.concatenate(split3(placed), axis=0), out_mat, preferred_element_type=F32)
        both = both[0:32] + both[32:64] + both[64:96]
        return both[:, 0:128], both[:, 128:256]

    def pack(message):
        kept = jnp.where(in_group, message, 0.0)
        out = kept[0:4]
        for g in range(1, 8):
            out = out + kept[4 * g : 4 * g + 4]
        return out

    def unpack(message):
        tall = jnp.where(in_group, jnp.concatenate([message] * 8, axis=0), 0.0)
        both = jnp.dot(jnp.concatenate(split3(tall), axis=0), place, preferred_element_type=F32)
        return both[0:32] + both[32:64] + both[64:96]

    def exchange(slot, parts):
        count = len(parts)
        buf_ref = buf_refs[slot]
        own_rows = send_ref.at[slot, 0 : 4 * count]
        for i, part in enumerate(parts):
            send_ref[slot, 4 * i : 4 * i + 4] = part
            buf_ref[me, 4 * i : 4 * i + 4] = part

        def send(k, carry):
            pltpu.make_async_remote_copy(
                src_ref=own_rows,
                dst_ref=buf_ref.at[me],
                send_sem=send_sem.at[slot],
                recv_sem=recv_sem.at[slot],
                device_id=coords(lax.rem(me + k, devices)),
                device_id_type=pl.DeviceIdType.MESH,
            ).start()
            return carry

        lax.fori_loop(1, devices, send, 0)
        every = buf_ref.at[pl.ds(0, devices - 1)]
        pltpu.make_async_copy(every, every, recv_sem.at[slot]).wait()
        pltpu.make_async_copy(every, every, send_sem.at[slot]).wait()
        from_upper = [buf_ref[upper_ref[0, i]] for i in range(2)]
        from_lower = [buf_ref[lower_ref[0, i]] for i in range(2)]
        out = []
        for i in range(count):
            rows = slice(4 * i, 4 * i + 4)
            mixed = jnp.where(
                slot4 < 4,
                from_upper[0][rows],
                jnp.where(
                    slot4 < 8, from_upper[1][rows], jnp.where(slot4 < 12, from_lower[0][rows], from_lower[1][rows])
                ),
            )
            out.append(unpack(mixed))
        return out

    spare = (lane4 // 16 == 6) & (iota((4, LANES), 0) == 1)

    diag_part, diag_out = collect(from_rows(diag_ref[...]))
    padded = jnp.concatenate([lrow_ref[...], jnp.zeros((LANES - elems, 256), F32)], axis=0)
    turned = jnp.concatenate([padded[:, 0:128].T, padded[:, 128:256].T], axis=0)
    slices = [jnp.concatenate([turned[253:256], turned[0:22]], axis=0)]
    slices += [turned[25 * j - 3 : 25 * j + 22] for j in range(1, 6)]
    load_part, load_out = collect(by_face(slices))
    pl.semaphore_wait(barrier, devices - 1)
    got = exchange(0, [pack(load_out), pack(diag_out)])
    live = (lane32 < FACE_DEV + REMOTE) & (sub32 < FACE_DOFS)
    residual = jnp.where(live, load_part + got[0], 0.0)
    weights = jnp.where(live, 1.0 / jnp.where(live, diag_part + got[1], 1.0), 0.0)

    trace = jnp.zeros((32, LANES), F32)
    direction = jnp.zeros((32, LANES), F32)
    image = jnp.zeros((32, LANES), F32)
    rz_now = None
    step = None
    row_lane = iota((ROWS, LANES), 1)
    row_elem = jnp.where(row_lane < 48, row_lane % 16, -1)
    for iteration in range(ITERS):
        precond = residual * weights
        values = spread(precond)
        cols = columns(values)
        total = jnp.zeros((ROWS, LANES), F32)
        for e in range(elems):
            rows = slice(ROWS * e, ROWS * e + ROWS)
            product = jnp.dot(shi_ref[rows], cols, preferred_element_type=F32)
            product = product + jnp.dot(slo_ref[rows], cols, preferred_element_type=F32)
            total = jnp.where(row_elem == e, product, total)
        total = total + pltpu.roll(total, LANES - 16, 1) + pltpu.roll(total, LANES - 32, 1)
        result = from_rows(total)
        flat = values[:, 0:128] + values[:, 128:256] + values[:, 256:384]
        curve_part = jnp.sum(jnp.where(lane32 < 6 * elems, flat * result, 0.0))
        rz_part = jnp.sum(jnp.where(owned, residual * precond, 0.0))
        part, out = collect(result)
        message = pack(out)
        message = jnp.where(spare, jnp.where(slot4 == 0, rz_part, jnp.where(slot4 == 1, curve_part, 0.0)), message)
        slot = iteration + 1
        got = exchange(slot, [message])[0]

        def add(d, carry):
            return carry + buf_refs[slot][d]

        sums = lax.fori_loop(0, devices, add, jnp.zeros((4, LANES), F32))
        rz_next = jnp.sum(jnp.where(spare & (slot4 == 0), sums, 0.0), keepdims=True)
        curve = jnp.sum(jnp.where(spare & (slot4 == 1), sums, 0.0), keepdims=True)
        mapped = jnp.where(live, part + got, 0.0)
        if iteration == 0:
            step = rz_next / curve
            direction, image = precond, mapped
        else:
            ratio = rz_next / rz_now
            step = rz_next / (curve - ratio * rz_next / step)
            direction = precond + ratio * direction
            image = mapped + ratio * image
        rz_now = rz_next
        trace = trace + step * direction
        residual = residual - step * image
    trace_ref[...] = trace[0:FACE_DOFS, 0:FACE_DEV]
    resid_ref[...] = residual[0:FACE_DOFS, 0:FACE_DEV]


def on_device(
    sizes, basis_mats, coeffs, element_loads, elem_faces, orient_codes, shared_owned, shared_remote, lower_peers, upper_peers
):
    elems, terms = coeffs.shape
    vmem = pl.BlockSpec(memory_space=pltpu.VMEM)
    smem = pl.BlockSpec(memory_space=pltpu.SMEM)
    loads = jnp.pad(element_loads, ((0, 0), (0, 384 - LOCAL_DOFS)))
    shi, slo, diag, lrow = pl.pallas_call(
        functools.partial(condense_kernel, elems, terms),
        out_shape=(
            jax.ShapeDtypeStruct((elems * ROWS, 256), BF),
            jax.ShapeDtypeStruct((elems * ROWS, 256), BF),
            jax.ShapeDtypeStruct((ROWS, LANES), F32),
            jax.ShapeDtypeStruct((elems, 256), F32),
        ),
        in_specs=[smem, vmem, vmem],
        out_specs=(vmem, vmem, vmem, vmem),
        scratch_shapes=[
            [pltpu.VMEM((elems // WAYS, 288, 384), F32)] * WAYS,
            pltpu.VMEM((elems, NB, LANES), BF),
            [pltpu.VMEM((LANES, 384), BF)] * WAYS,
        ],
        compiler_params=pltpu.CompilerParams(vmem_limit_bytes=40 * 1024 * 1024),
        name="condense",
    )(coeffs, basis_mats, loads)

    def lane_row(values, fill):
        flat = values.reshape(1, -1)
        return jnp.pad(flat, ((0, 0), (0, LANES - flat.shape[1])), constant_values=fill)

    own = shared_owned.reshape(-1)
    far = FACE_DEV + shared_remote.reshape(-1)
    ints = jnp.concatenate(
        [
            lane_row(elem_faces.T, -1),
            lane_row(orient_codes.T, 0),
            jnp.tile(jnp.concatenate([own, far]), 8)[None],
            jnp.tile(jnp.concatenate([far, own]), 8)[None],
            jnp.zeros((4, LANES), jnp.int32),
        ],
        axis=0,
    )
    stack = permute_stack()
    devices = sizes[0] * sizes[1]
    return pl.pallas_call(
        functools.partial(cg_kernel, ("gx", "gy"), sizes, elems),
        out_shape=(
            jax.ShapeDtypeStruct((FACE_DOFS, FACE_DEV), F32),
            jax.ShapeDtypeStruct((FACE_DOFS, FACE_DEV), F32),
        ),
        in_specs=[smem, smem] + [vmem] * 7,
        out_specs=(vmem, vmem),
        scratch_shapes=[
            [pltpu.VMEM((devices, 8 if i == 0 else 4, LANES), F32) for i in range(ITERS + 1)],
            pltpu.VMEM((ITERS + 1, 8, LANES), F32),
            pltpu.SemaphoreType.DMA((ITERS + 1,)),
            pltpu.SemaphoreType.DMA((ITERS + 1,)),
        ],
        compiler_params=pltpu.CompilerParams(
            collective_id=0, has_side_effects=True, vmem_limit_bytes=48 * 1024 * 1024
        ),
        name="solve",
    )(
        upper_peers, lower_peers, ints, jnp.asarray(stack, BF), jnp.asarray(stack.T, BF), shi, slo, diag, lrow
    )


def solution(mesh):
    row = P(("gx", "gy"), None)
    cube = P(("gx", "gy"), None, None)
    sizes = (mesh.shape["gx"], mesh.shape["gy"])
    return jax.shard_map(
        functools.partial(on_device, sizes),
        mesh=mesh,
        in_specs=(P(), row, row, row, row, cube, cube, row, row),
        out_specs=(P(None, ("gx", "gy")), P(None, ("gx", "gy"))),
        check_vma=False,
    )
```

```python
import functools

import jax
import jax.numpy as jnp
import numpy as np
from jax import lax
from jax.experimental import pallas as pl
from jax.experimental.pallas import tpu as pltpu
from jax.sharding import PartitionSpec as P

SIDE = 5
FACE_DOFS = 25
CELL_DOFS = 125
TRACE_DOFS = 150
LOCAL_DOFS = 275
ITERS = 4
FACE_DEV = 64
SHARED = 4
REMOTE = 8
LANES = 128
ROWS = 160
NB = 32
CUTS = (0, 64, 128, 200, 275)
WAYS = 4
BF = jnp.bfloat16
F32 = jnp.float32


def orient_table():
    n = SIDE
    table = np.zeros((8, n * n), np.int32)
    for code in range(8):
        for a in range(n):
            for b in range(n):
                a2, b2 = (b, a) if code & 1 else (a, b)
                if code & 2:
                    a2 = n - 1 - a2
                if code & 4:
                    b2 = n - 1 - b2
                table[code, a * n + b] = a2 * n + b2
    return table


def permute_stack():
    table = orient_table()
    out = np.zeros((32, 256), np.float32)
    for code in range(8):
        for q in range(FACE_DOFS):
            out[q, 32 * code + table[code, q]] = 1.0
    return out


def iota(shape, dim):
    return lax.broadcasted_iota(jnp.int32, shape, dim)


def hi_part(x):
    return x.astype(BF).astype(F32)


def pack_lanes(x, source):
    lane = iota(x.shape, 1)

    def at(place):
        shift = (place - source) % LANES
        return x if shift == 0 else pltpu.roll(x, shift, 1)

    x0, x1, x2 = at(0), at(NB), at(2 * NB)
    packed = jnp.where(lane < NB, x0, jnp.where(lane < 2 * NB, x1 - hi_part(x1), x2))
    return jnp.where(lane < 3 * NB, packed, 0.0).astype(BF)


def pack_rows(x):
    high = x.astype(BF)
    low = (x - high.astype(F32)).astype(BF)
    return jnp.concatenate([high, high, low, jnp.zeros_like(high)], axis=0)


def inverse2(m):
    (a, b), (c, d) = m
    scale = 1.0 / (a * d - b * c)
    return (d * scale, -b * scale), (-c * scale, a * scale)


def times2(m, n):
    return tuple(tuple(m[i][0] * n[0][j] + m[i][1] * n[1][j] for j in range(len(n[0]))) for i in range(2))


def minus2(m, n):
    return tuple(tuple(a - b for a, b in zip(x, y)) for x, y in zip(m, n))


def invert_blocks(tiles):
    lane = iota((8, LANES), 1)
    sub = iota((8, LANES), 0)
    inside = lane % NB
    first = lane - inside
    for k in range(0, NB, 4):
        tk, sk = k // 8, k % 8
        here = inside // 4 == k // 4
        for g in range(len(tiles)):
            group = tiles[g]
            columns = [
                [jnp.take_along_axis(group[t], first + (k + m), axis=1) for t in range(4)] for m in range(4)
            ]

            def spread(value, i):
                return jnp.broadcast_to(value[sk + i : sk + i + 1, :], (8, LANES))

            def block(i, j):
                return tuple(tuple(spread(columns[n][tk], m) for n in (j, j + 1)) for m in (i, i + 1))

            rows = [
                (jnp.where(here, jnp.where(inside == k + m, 1.0, 0.0), spread(group[tk], m)),) for m in range(4)
            ]
            a_inv = inverse2(block(0, 0))
            c = block(2, 0)
            t_block = times2(a_inv, block(0, 2))
            s_inv = inverse2(minus2(block(2, 2), times2(c, t_block)))
            upper = times2(a_inv, (rows[0], rows[1]))
            lower = times2(s_inv, minus2((rows[2], rows[3]), times2(c, upper)))
            upper = minus2(upper, times2(t_block, lower))
            fresh_rows = [upper[0][0], upper[1][0], lower[0][0], lower[1][0]]
            fresh = []
            for t in range(4):
                value = jnp.where(here, 0.0, group[t])
                value = value - (
                    (columns[0][t] * fresh_rows[0] + columns[1][t] * fresh_rows[1])
                    + (columns[2][t] * fresh_rows[2] + columns[3][t] * fresh_rows[3])
                )
                if t == tk:
                    for m in range(4):
                        value = jnp.where(sub == sk + m, fresh_rows[m], value)
                fresh.append(value)
            tiles[g] = fresh
    return tiles


def condense(elems, terms, coef_ref, basis_ref, arrived, load_ref, shi_ref, slo_ref, diag_ref, lrow_ref, x_refs, d_ref, r_refs):
    lane8 = iota((8, LANES), 1)
    sub8 = iota((8, LANES), 0)
    tail = LOCAL_DOFS - 256

    def combine(row_slice, count, emit):
        parts = [
            [basis_ref[k, row_slice, 0:128], basis_ref[k, row_slice, 128:256], basis_ref[k, row_slice, 256:LOCAL_DOFS]]
            for k in range(terms)
        ]
        for e in range(elems):
            total = None
            for k in range(terms):
                scaled = [coef_ref[e, k] * part for part in parts[k]]
                total = scaled if total is None else [a + b for a, b in zip(total, scaled)]
            t0, t1, t2 = total
            t2 = jnp.concatenate([t2, jnp.zeros((count, LANES - tail), F32)], axis=1)
            if count < 8:
                t0, t1, t2 = (
                    jnp.concatenate([t, jnp.zeros((8 - count, LANES), F32)], axis=0) for t in (t0, t1, t2)
                )
            emit(e, t0, t1, t2)

    def put(e, start, *tiles):
        for i, tile in enumerate(tiles):
            x_refs[e % WAYS][e // WAYS, pl.ds(start, 8), LANES * i : LANES * i + LANES] = tile

    def put_inner(e, start, t0, t1, t2, edge):
        inner = lane8 < CELL_DOFS
        moved = jnp.where(inner, t2, t0)
        kept = jnp.where(inner, t0, 0.0)
        if edge:
            good = sub8 + 120 < CELL_DOFS
            kept = jnp.where(good, kept, jnp.where(sub8 + 120 == lane8, 1.0, 0.0))
            t1 = jnp.where(good, t1, 0.0)
            moved = jnp.where(good, moved, 0.0)
        put(e, start, kept, t1, moved)

    def put_outer(e, start, t0, t1, t2):
        inner = lane8 < CELL_DOFS
        put(e, start, jnp.where(inner, t0, 0.0), t1, jnp.where(inner, t2, t0))

    def inner_rows(t):
        start = pl.multiple_of(t * 8, 8)
        combine(pl.ds(start, 8), 8, lambda e, a, b, c: put_inner(e, start, a, b, c, False))

    def outer_rows(t):
        start = pl.multiple_of(t * 8, 8)
        combine(pl.ds(start, 8), 8, lambda e, a, b, c: put_outer(e, start + 8, a, b, c))

    arrived(0)
    pl.loop(0, CUTS[1] // 8)(inner_rows)
    arrived(1)
    pl.loop(CUTS[1] // 8, 15)(inner_rows)

    def edge_rows(e, t0, t1, t2):
        put_inner(e, 120, t0, t1, t2, True)
        first = sub8 == 0

        def with_load(tile, lo):
            row = load_ref[e : e + 1, lo : min(lo + LANES, LOCAL_DOFS)]
            if row.shape[1] < LANES:
                row = jnp.concatenate([row, jnp.zeros((1, LANES - row.shape[1]), F32)], axis=1)
            return jnp.where(first, jnp.broadcast_to(row, (8, LANES)), tile)

        put_outer(e, 128, with_load(t0, 0), with_load(t1, 128), with_load(t2, 256))

    combine(pl.ds(120, 8), 8, edge_rows)

    arrived(2)
    pl.loop(16, CUTS[3] // 8)(outer_rows)
    arrived(3)
    pl.loop(CUTS[3] // 8, 34)(outer_rows)
    combine(pl.ds(272, 3), 3, lambda e, a, b, c: put_outer(e, 280, a, b, c))

    groups = elems // 4
    lane32 = iota((NB, LANES), 1)
    for b in range(4):
        rows = slice(NB * b, NB * b + NB)
        tiles = []
        for g in range(groups):
            whole = jnp.zeros((NB, LANES), F32)
            for q in range(4):
                part = x_refs[q][g, rows, 0:128]
                shift = (NB * (q - b)) % LANES
                if shift:
                    part = pltpu.roll(part, shift, 1)
                whole = jnp.where(lane32 // NB == q, part, whole)
            tiles.append([whole[8 * t : 8 * t + 8] for t in range(4)])
        tiles = invert_blocks(tiles)
        for g in range(groups):
            whole = jnp.concatenate(tiles[g], axis=0)
            for q in range(4):
                d_ref[g * 4 + q] = pack_lanes(whole, NB * q)
        lo = 0 if b < 3 else LANES

        below = slice(NB * (b + 1), 288)

        @pl.loop(0, groups)
        def _(g):
            for q in range(WAYS):
                scaled = jnp.dot(
                    d_ref[g * WAYS + q], pack_rows(x_refs[q][g, rows, lo:384]), preferred_element_type=F32
                )
                r_refs[q][:, lo:384] = pack_rows(scaled)
            for q in range(WAYS):
                lhs = pack_lanes(x_refs[q][g, below, 0:128], NB * b)
                update = jnp.dot(lhs, r_refs[q][:, lo:384], preferred_element_type=F32)
                x_refs[q][g, below, lo:384] = x_refs[q][g, below, lo:384] - update

    diag_ref[...] = jnp.zeros_like(diag_ref)
    lane_w = iota((ROWS, 256), 1)
    on_diag = (iota((ROWS, 256), 0) + 248) % 256 == lane_w
    lane_t = iota((ROWS, LANES), 1)

    @pl.loop(0, groups)
    def _(g):
        for q in range(WAYS):
            e = g * WAYS + q
            s = x_refs[q][g, 128:288, 128:384]
            high = s.astype(BF)
            start = pl.multiple_of(e * ROWS, 32)
            shi_ref[pl.ds(start, ROWS), :] = high
            slo_ref[pl.ds(start, ROWS), :] = (s - high.astype(F32)).astype(BF)
            only = jnp.where(on_diag, s, 0.0)
            column = jnp.sum(only[:, 0:128] + only[:, 128:256], axis=1, keepdims=True)
            diag_ref[...] = jnp.where(lane_t == e, column, diag_ref[...])
            lrow_ref[pl.ds(e, 1), :] = s[0:1, :]


def split3(x):
    a = x.astype(BF)
    rest = x - a.astype(F32)
    b = rest.astype(BF)
    c = (rest - b.astype(F32)).astype(BF)
    return a, b, c


def kernel(
    mesh_names, sizes, elems, terms, coef_ref, upper_ref, lower_ref, owned_ref, remote_ref, basis_hbm, load_ref, face_ref,
    code_ref, perm_ref, permt_ref, trace_ref, resid_ref, basis_ref, shi_ref, slo_ref, diag_ref, lrow_ref, x_refs, d_ref,
    r_refs, buf_refs, send_ref, basis_sem, send_sem, recv_sem,
):
    devices = sizes[0] * sizes[1]
    me = lax.axis_index(mesh_names[0]) * sizes[1] + lax.axis_index(mesh_names[1])

    def chunk(i):
        rows = slice(CUTS[i], CUTS[i + 1])
        return pltpu.make_async_copy(basis_hbm.at[:, rows, :], basis_ref.at[:, rows, :], basis_sem.at[i])

    for i in range(4):
        chunk(i).start()

    def coords(d):
        return (d // sizes[1], lax.rem(d, sizes[1]))

    barrier = pltpu.get_barrier_semaphore()

    def greet(k, carry):
        pl.semaphore_signal(
            barrier, inc=1, device_id=coords(lax.rem(me + k, devices)), device_id_type=pl.DeviceIdType.MESH
        )
        return carry

    lax.fori_loop(1, devices, greet, 0)

    condense(
        elems, terms, coef_ref, basis_ref, lambda i: chunk(i).wait(), load_ref, shi_ref, slo_ref, diag_ref, lrow_ref,
        x_refs, d_ref, r_refs,
    )

    square = (LANES, LANES)
    sub = iota(square, 0)
    lane1 = iota((1, LANES), 1)

    def in_lanes(ref, fill):
        wide = jnp.concatenate([ref[...].astype(F32), jnp.zeros((elems, LANES - 6), F32)], axis=1)
        turned = jnp.concatenate([wide, jnp.zeros((LANES - elems, LANES), F32)], axis=0).T
        out = jnp.full((1, LANES), fill, F32)
        for j in range(6):
            row = turned[j : j + 1]
            if j:
                row = pltpu.roll(row, 16 * j, 1)
            out = jnp.where(lane1 // 16 == j, row, out)
        return out

    def listed(first, second):
        out = jnp.zeros((1, LANES), jnp.int32)
        for at, (ref, base) in enumerate((first, second)):
            for i in range(2):
                for k in range(SHARED):
                    out = jnp.where(lane1 % 16 == 8 * at + SHARED * i + k, base + ref[0, i, k], out)
        return out

    own, far = (owned_ref, 0), (remote_ref, FACE_DEV)
    inc_t = jnp.where(sub.astype(F32) == in_lanes(face_ref, -1.0), 1.0, 0.0)
    inc = inc_t.T
    sel = jnp.where(sub == listed(own, far), 1.0, 0.0).astype(BF)
    place = jnp.where(sub == listed(far, own), 1.0, 0.0).T.astype(BF)
    inc_t = inc_t.astype(BF)
    inc = inc.astype(BF)
    inc_sel = jnp.dot(inc, sel, preferred_element_type=F32).astype(BF)
    out_mat = jnp.concatenate([inc, inc_sel], axis=1)
    perm = perm_ref[...]
    perm_t = permt_ref[...]
    code = in_lanes(code_ref, 0.0)
    lane32 = iota((32, LANES), 1)
    sub32 = iota((32, LANES), 0)
    in_group = lane32 // 16 == sub32 // 4
    lane4 = iota((4, LANES), 1)
    slot4 = lane4 % 16
    owned = lane32 < FACE_DEV

    def spread(field):
        a, b, c = split3(field)
        got = jnp.dot(jnp.concatenate([a, b, c], axis=0), inc_t, preferred_element_type=F32)
        pieces = []
        for s in range(3):
            part = got[32 * s : 32 * s + 32]
            pieces.append(
                jnp.concatenate([jnp.where(code == o, part, 0.0) for o in range(8)], axis=0).astype(BF)
            )
        return jnp.dot(perm, jnp.concatenate(pieces, axis=1), preferred_element_type=F32)

    def columns(values):
        blocks = []
        for j in range(6):
            block = jnp.zeros((32, LANES), F32)
            for s in range(3):
                part = values[:, LANES * s : LANES * s + LANES]
                shift = (16 * s - 16 * j) % LANES
                if shift:
                    part = pltpu.roll(part, shift, 1)
                block = jnp.where(lane32 // 16 == s, part, block)
            blocks.append(block)
        return jnp.concatenate(
            [blocks[0][3:25]] + [x[0:25] for x in blocks[1:]] + [jnp.zeros((106, LANES), F32), blocks[0][0:3]], axis=0
        ).astype(BF)

    def by_face(slices):
        out = jnp.zeros((32, LANES), F32)
        for j in range(6):
            part = jnp.concatenate([slices[j], jnp.zeros((7, LANES), F32)], axis=0)
            if j:
                part = pltpu.roll(part, 16 * j, 1)
            out = jnp.where(lane32 // 16 == j, part, out)
        return out

    def from_rows(t):
        return by_face([t[5 + 25 * j : 30 + 25 * j] for j in range(6)])

    def collect(values):
        turned = jnp.dot(perm_t, jnp.concatenate(split3(values), axis=1), preferred_element_type=F32)
        turned = turned[:, 0:128] + turned[:, 128:256] + turned[:, 256:384]
        placed = jnp.zeros((32, LANES), F32)
        for o in range(8):
            placed = jnp.where(code == o, turned[32 * o : 32 * o + 32], placed)
        both = jnp.dot(jnp.concatenate(split3(placed), axis=0), out_mat, preferred_element_type=F32)
        both = both[0:32] + both[32:64] + both[64:96]
        return both[:, 0:128], both[:, 128:256]

    def pack(message):
        kept = jnp.where(in_group, message, 0.0)
        out = kept[0:4]
        for g in range(1, 8):
            out = out + kept[4 * g : 4 * g + 4]
        return out

    def unpack(message):
        tall = jnp.where(in_group, jnp.concatenate([message] * 8, axis=0), 0.0)
        both = jnp.dot(jnp.concatenate(split3(tall), axis=0), place, preferred_element_type=F32)
        return both[0:32] + both[32:64] + both[64:96]

    def exchange(slot, parts):
        count = len(parts)
        buf_ref = buf_refs[slot]
        own_rows = send_ref.at[slot, 0 : 4 * count]
        for i, part in enumerate(parts):
            send_ref[slot, 4 * i : 4 * i + 4] = part
            buf_ref[me, 4 * i : 4 * i + 4] = part

        def send(k, carry):
            pltpu.make_async_remote_copy(
                src_ref=own_rows,
                dst_ref=buf_ref.at[me],
                send_sem=send_sem.at[slot],
                recv_sem=recv_sem.at[slot],
                device_id=coords(lax.rem(me + k, devices)),
                device_id_type=pl.DeviceIdType.MESH,
            ).start()
            return carry

        lax.fori_loop(1, devices, send, 0)
        every = buf_ref.at[pl.ds(0, devices - 1)]
        pltpu.make_async_copy(every, every, recv_sem.at[slot]).wait()
        pltpu.make_async_copy(every, every, send_sem.at[slot]).wait()
        from_upper = [buf_ref[upper_ref[0, i]] for i in range(2)]
        from_lower = [buf_ref[lower_ref[0, i]] for i in range(2)]
        out = []
        for i in range(count):
            rows = slice(4 * i, 4 * i + 4)
            mixed = jnp.where(
                slot4 < 4,
                from_upper[0][rows],
                jnp.where(
                    slot4 < 8, from_upper[1][rows], jnp.where(slot4 < 12, from_lower[0][rows], from_lower[1][rows])
                ),
            )
            out.append(unpack(mixed))
        return out

    spare = (lane4 // 16 == 6) & (iota((4, LANES), 0) == 1)

    diag_part, diag_out = collect(from_rows(diag_ref[...]))
    padded = jnp.concatenate([lrow_ref[...], jnp.zeros((LANES - elems, 256), F32)], axis=0)
    turned = jnp.concatenate([padded[:, 0:128].T, padded[:, 128:256].T], axis=0)
    slices = [jnp.concatenate([turned[253:256], turned[0:22]], axis=0)]
    slices += [turned[25 * j - 3 : 25 * j + 22] for j in range(1, 6)]
    load_part, load_out = collect(by_face(slices))
    pl.semaphore_wait(barrier, devices - 1)
    got = exchange(0, [pack(load_out), pack(diag_out)])
    live = (lane32 < FACE_DEV + REMOTE) & (sub32 < FACE_DOFS)
    residual = jnp.where(live, load_part + got[0], 0.0)
    weights = jnp.where(live, 1.0 / jnp.where(live, diag_part + got[1], 1.0), 0.0)

    trace = jnp.zeros((32, LANES), F32)
    direction = jnp.zeros((32, LANES), F32)
    image = jnp.zeros((32, LANES), F32)
    rz_now = None
    step = None
    row_lane = iota((ROWS, LANES), 1)
    row_elem = jnp.where(row_lane < 48, row_lane % 16, -1)
    for iteration in range(ITERS):
        precond = residual * weights
        values = spread(precond)
        cols = columns(values)
        total = jnp.zeros((ROWS, LANES), F32)
        for e in range(elems):
            rows = slice(ROWS * e, ROWS * e + ROWS)
            product = jnp.dot(shi_ref[rows], cols, preferred_element_type=F32)
            product = product + jnp.dot(slo_ref[rows], cols, preferred_element_type=F32)
            total = jnp.where(row_elem == e, product, total)
        total = total + pltpu.roll(total, LANES - 16, 1) + pltpu.roll(total, LANES - 32, 1)
        result = from_rows(total)
        flat = values[:, 0:128] + values[:, 128:256] + values[:, 256:384]
        curve_part = jnp.sum(jnp.where(lane32 < 6 * elems, flat * result, 0.0))
        rz_part = jnp.sum(jnp.where(owned, residual * precond, 0.0))
        part, out = collect(result)
        message = pack(out)
        message = jnp.where(spare, jnp.where(slot4 == 0, rz_part, jnp.where(slot4 == 1, curve_part, 0.0)), message)
        slot = iteration + 1
        got = exchange(slot, [message])[0]

        def add(d, carry):
            return carry + buf_refs[slot][d]

        sums = lax.fori_loop(0, devices, add, jnp.zeros((4, LANES), F32))
        rz_next = jnp.sum(jnp.where(spare & (slot4 == 0), sums, 0.0), keepdims=True)
        curve = jnp.sum(jnp.where(spare & (slot4 == 1), sums, 0.0), keepdims=True)
        mapped = jnp.where(live, part + got, 0.0)
        if iteration == 0:
            step = rz_next / curve
            direction, image = precond, mapped
        else:
            ratio = rz_next / rz_now
            step = rz_next / (curve - ratio * rz_next / step)
            direction = precond + ratio * direction
            image = mapped + ratio * image
        rz_now = rz_next
        trace = trace + step * direction
        residual = residual - step * image
    trace_ref[...] = trace[0:FACE_DOFS, 0:FACE_DEV]
    resid_ref[...] = residual[0:FACE_DOFS, 0:FACE_DEV]


def on_device(
    sizes, basis_mats, coeffs, element_loads, elem_faces, orient_codes, shared_owned, shared_remote, lower_peers, upper_peers
):
    elems, terms = coeffs.shape
    vmem = pl.BlockSpec(memory_space=pltpu.VMEM)
    smem = pl.BlockSpec(memory_space=pltpu.SMEM)
    stack = permute_stack()
    devices = sizes[0] * sizes[1]
    return pl.pallas_call(
        functools.partial(kernel, ("gx", "gy"), sizes, elems, terms),
        out_shape=(
            jax.ShapeDtypeStruct((FACE_DOFS, FACE_DEV), F32),
            jax.ShapeDtypeStruct((FACE_DOFS, FACE_DEV), F32),
        ),
        in_specs=[smem] * 5 + [pl.BlockSpec(memory_space=pltpu.HBM)] + [vmem] * 5,
        out_specs=(vmem, vmem),
        scratch_shapes=[
            pltpu.VMEM((terms, LOCAL_DOFS, LOCAL_DOFS), F32),
            pltpu.VMEM((elems * ROWS, 256), BF),
            pltpu.VMEM((elems * ROWS, 256), BF),
            pltpu.VMEM((ROWS, LANES), F32),
            pltpu.VMEM((elems, 256), F32),
            [pltpu.VMEM((elems // WAYS, 288, 384), F32)] * WAYS,
            pltpu.VMEM((elems, NB, LANES), BF),
            [pltpu.VMEM((LANES, 384), BF)] * WAYS,
            [pltpu.VMEM((devices, 8 if i == 0 else 4, LANES), F32) for i in range(ITERS + 1)],
            pltpu.VMEM((ITERS + 1, 8, LANES), F32),
            pltpu.SemaphoreType.DMA((4,)),
            pltpu.SemaphoreType.DMA((ITERS + 1,)),
            pltpu.SemaphoreType.DMA((ITERS + 1,)),
        ],
        compiler_params=pltpu.CompilerParams(
            collective_id=0, has_side_effects=True, vmem_limit_bytes=56 * 1024 * 1024
        ),
        name="hdg",
    )(
        coeffs, upper_peers, lower_peers, shared_owned, shared_remote, basis_mats, element_loads, elem_faces, orient_codes,
        jnp.asarray(stack, BF), jnp.asarray(stack.T, BF),
    )


def solution(mesh):
    row = P(("gx", "gy"), None)
    cube = P(("gx", "gy"), None, None)
    sizes = (mesh.shape["gx"], mesh.shape["gy"])
    return jax.shard_map(
        functools.partial(on_device, sizes),
        mesh=mesh,
        in_specs=(P(), row, row, row, row, cube, cube, row, row),
        out_specs=(P(None, ("gx", "gy")), P(None, ("gx", "gy"))),
        check_vma=False,
    )
```

```python
import functools

import jax
import jax.numpy as jnp
import numpy as np
from jax import lax
from jax.experimental import pallas as pl
from jax.experimental.pallas import tpu as pltpu
from jax.sharding import PartitionSpec as P

SIDE = 5
FACE_DOFS = 25
CELL_DOFS = 125
TRACE_DOFS = 150
LOCAL_DOFS = 275
ITERS = 4
FACE_DEV = 64
SHARED = 4
REMOTE = 8
LANES = 128
ROWS = 160
NB = 32
CUTS = (0, 64, 128, 200, 275)
WAYS = 4
BF = jnp.bfloat16
F32 = jnp.float32


def orient_table():
    n = SIDE
    table = np.zeros((8, n * n), np.int32)
    for code in range(8):
        for a in range(n):
            for b in range(n):
                a2, b2 = (b, a) if code & 1 else (a, b)
                if code & 2:
                    a2 = n - 1 - a2
                if code & 4:
                    b2 = n - 1 - b2
                table[code, a * n + b] = a2 * n + b2
    return table


def permute_stack():
    table = orient_table()
    out = np.zeros((32, 256), np.float32)
    for code in range(8):
        for q in range(FACE_DOFS):
            out[q, 32 * code + table[code, q]] = 1.0
    return out


def iota(shape, dim):
    return lax.broadcasted_iota(jnp.int32, shape, dim)


def hi_part(x):
    return x.astype(BF).astype(F32)


def pack_lanes(x, source):
    lane = iota(x.shape, 1)

    def at(place):
        shift = (place - source) % LANES
        return x if shift == 0 else pltpu.roll(x, shift, 1)

    x0, x1, x2 = at(0), at(NB), at(2 * NB)
    packed = jnp.where(lane < NB, x0, jnp.where(lane < 2 * NB, x1 - hi_part(x1), x2))
    return jnp.where(lane < 3 * NB, packed, 0.0).astype(BF)


def pack_rows(x):
    high = x.astype(BF)
    low = (x - high.astype(F32)).astype(BF)
    return jnp.concatenate([high, high, low, jnp.zeros_like(high)], axis=0)


def inverse2(m):
    (a, b), (c, d) = m
    scale = 1.0 / (a * d - b * c)
    return (d * scale, -b * scale), (-c * scale, a * scale)


def times2(m, n):
    return tuple(tuple(m[i][0] * n[0][j] + m[i][1] * n[1][j] for j in range(len(n[0]))) for i in range(2))


def minus2(m, n):
    return tuple(tuple(a - b for a, b in zip(x, y)) for x, y in zip(m, n))


def invert_blocks(tiles):
    lane = iota((8, LANES), 1)
    sub = iota((8, LANES), 0)
    inside = lane % NB
    first = lane - inside
    for k in range(0, NB, 4):
        tk, sk = k // 8, k % 8
        here = inside // 4 == k // 4
        for g in range(len(tiles)):
            group = tiles[g]
            columns = [
                [jnp.take_along_axis(group[t], first + (k + m), axis=1) for t in range(4)] for m in range(4)
            ]

            def spread(value, i):
                return jnp.broadcast_to(value[sk + i : sk + i + 1, :], (8, LANES))

            def block(i, j):
                return tuple(tuple(spread(columns[n][tk], m) for n in (j, j + 1)) for m in (i, i + 1))

            rows = [
                (jnp.where(here, jnp.where(inside == k + m, 1.0, 0.0), spread(group[tk], m)),) for m in range(4)
            ]
            a_inv = inverse2(block(0, 0))
            c = block(2, 0)
            t_block = times2(a_inv, block(0, 2))
            s_inv = inverse2(minus2(block(2, 2), times2(c, t_block)))
            upper = times2(a_inv, (rows[0], rows[1]))
            lower = times2(s_inv, minus2((rows[2], rows[3]), times2(c, upper)))
            upper = minus2(upper, times2(t_block, lower))
            fresh_rows = [upper[0][0], upper[1][0], lower[0][0], lower[1][0]]
            fresh = []
            for t in range(4):
                value = jnp.where(here, 0.0, group[t])
                value = value - (
                    (columns[0][t] * fresh_rows[0] + columns[1][t] * fresh_rows[1])
                    + (columns[2][t] * fresh_rows[2] + columns[3][t] * fresh_rows[3])
                )
                if t == tk:
                    for m in range(4):
                        value = jnp.where(sub == sk + m, fresh_rows[m], value)
                fresh.append(value)
            tiles[g] = fresh
    return tiles


def condense(elems, terms, coef_ref, basis_ref, arrived, load_ref, shi_ref, slo_ref, diag_ref, lrow_ref, x_refs, d_ref, r_refs):
    lane8 = iota((8, LANES), 1)
    sub8 = iota((8, LANES), 0)
    tail = LOCAL_DOFS - 256

    def combine(row_slice, count, emit):
        parts = [
            [basis_ref[k, row_slice, 0:128], basis_ref[k, row_slice, 128:256], basis_ref[k, row_slice, 256:LOCAL_DOFS]]
            for k in range(terms)
        ]
        for e in range(elems):
            total = None
            for k in range(terms):
                scaled = [coef_ref[e, k] * part for part in parts[k]]
                total = scaled if total is None else [a + b for a, b in zip(total, scaled)]
            t0, t1, t2 = total
            t2 = jnp.concatenate([t2, jnp.zeros((count, LANES - tail), F32)], axis=1)
            if count < 8:
                t0, t1, t2 = (
                    jnp.concatenate([t, jnp.zeros((8 - count, LANES), F32)], axis=0) for t in (t0, t1, t2)
                )
            emit(e, t0, t1, t2)

    def put(e, start, *tiles):
        for i, tile in enumerate(tiles):
            x_refs[e % WAYS][e // WAYS, pl.ds(start, 8), LANES * i : LANES * i + LANES] = tile

    def put_inner(e, start, t0, t1, t2, edge):
        inner = lane8 < CELL_DOFS
        moved = jnp.where(inner, t2, t0)
        kept = jnp.where(inner, t0, 0.0)
        if edge:
            good = sub8 + 120 < CELL_DOFS
            kept = jnp.where(good, kept, jnp.where(sub8 + 120 == lane8, 1.0, 0.0))
            t1 = jnp.where(good, t1, 0.0)
            moved = jnp.where(good, moved, 0.0)
        put(e, start, kept, t1, moved)

    def put_outer(e, start, t0, t1, t2):
        inner = lane8 < CELL_DOFS
        put(e, start, jnp.where(inner, t0, 0.0), t1, jnp.where(inner, t2, t0))

    def inner_rows(t):
        start = pl.multiple_of(t * 8, 8)
        combine(pl.ds(start, 8), 8, lambda e, a, b, c: put_inner(e, start, a, b, c, False))

    def outer_rows(t):
        start = pl.multiple_of(t * 8, 8)
        combine(pl.ds(start, 8), 8, lambda e, a, b, c: put_outer(e, start + 8, a, b, c))

    arrived(0)
    pl.loop(0, CUTS[1] // 8)(inner_rows)
    arrived(1)
    pl.loop(CUTS[1] // 8, 15)(inner_rows)

    def edge_rows(e, t0, t1, t2):
        put_inner(e, 120, t0, t1, t2, True)
        first = sub8 == 0

        def with_load(tile, lo):
            row = load_ref[e : e + 1, lo : min(lo + LANES, LOCAL_DOFS)]
            if row.shape[1] < LANES:
                row = jnp.concatenate([row, jnp.zeros((1, LANES - row.shape[1]), F32)], axis=1)
            return jnp.where(first, jnp.broadcast_to(row, (8, LANES)), tile)

        put_outer(e, 128, with_load(t0, 0), with_load(t1, 128), with_load(t2, 256))

    combine(pl.ds(120, 8), 8, edge_rows)

    arrived(2)
    pl.loop(16, CUTS[3] // 8)(outer_rows)
    arrived(3)
    pl.loop(CUTS[3] // 8, 34)(outer_rows)
    combine(pl.ds(272, 3), 3, lambda e, a, b, c: put_outer(e, 280, a, b, c))

    groups = elems // 4
    lane32 = iota((NB, LANES), 1)
    for b in range(4):
        rows = slice(NB * b, NB * b + NB)
        tiles = []
        for g in range(groups):
            whole = jnp.zeros((NB, LANES), F32)
            for q in range(4):
                part = x_refs[q][g, rows, 0:128]
                shift = (NB * (q - b)) % LANES
                if shift:
                    part = pltpu.roll(part, shift, 1)
                whole = jnp.where(lane32 // NB == q, part, whole)
            tiles.append([whole[8 * t : 8 * t + 8] for t in range(4)])
        tiles = invert_blocks(tiles)
        for g in range(groups):
            whole = jnp.concatenate(tiles[g], axis=0)
            for q in range(4):
                d_ref[g * 4 + q] = pack_lanes(whole, NB * q)
        lo = 0 if b < 3 else LANES

        below = slice(NB * (b + 1), 288)

        @pl.loop(0, groups)
        def _(g):
            for q in range(WAYS):
                scaled = jnp.dot(
                    d_ref[g * WAYS + q], pack_rows(x_refs[q][g, rows, lo:384]), preferred_element_type=F32
                )
                r_refs[q][:, lo:384] = pack_rows(scaled)
            for q in range(WAYS):
                lhs = pack_lanes(x_refs[q][g, below, 0:128], NB * b)
                update = jnp.dot(lhs, r_refs[q][:, lo:384], preferred_element_type=F32)
                x_refs[q][g, below, lo:384] = x_refs[q][g, below, lo:384] - update

    diag_ref[...] = jnp.zeros_like(diag_ref)
    lane_w = iota((ROWS, 256), 1)
    on_diag = (iota((ROWS, 256), 0) + 248) % 256 == lane_w
    lane_t = iota((ROWS, LANES), 1)

    @pl.loop(0, groups)
    def _(g):
        for q in range(WAYS):
            e = g * WAYS + q
            s = x_refs[q][g, 128:288, 128:384]
            high = s.astype(BF)
            start = pl.multiple_of(e * ROWS, 32)
            shi_ref[pl.ds(start, ROWS), :] = high
            slo_ref[pl.ds(start, ROWS), :] = (s - high.astype(F32)).astype(BF)
            only = jnp.where(on_diag, s, 0.0)
            column = jnp.sum(only[:, 0:128] + only[:, 128:256], axis=1, keepdims=True)
            diag_ref[...] = jnp.where(lane_t == e, column, diag_ref[...])
            lrow_ref[pl.ds(e, 1), :] = s[0:1, :]


def split3(x):
    a = x.astype(BF)
    rest = x - a.astype(F32)
    b = rest.astype(BF)
    c = (rest - b.astype(F32)).astype(BF)
    return a, b, c


def kernel(
    mesh_names, sizes, elems, terms, coef_ref, upper_ref, lower_ref, owned_ref, remote_ref, basis_hbm, load_ref, face_ref,
    code_ref, perm_ref, permt_ref, out_ref, basis_ref, shi_ref, slo_ref, diag_ref, lrow_ref, x_refs, d_ref,
    r_refs, buf_refs, send_ref, basis_sem, send_sem, recv_sem,
):
    devices = sizes[0] * sizes[1]
    me = lax.axis_index(mesh_names[0]) * sizes[1] + lax.axis_index(mesh_names[1])

    def chunk(i):
        rows = slice(CUTS[i], CUTS[i + 1])
        return pltpu.make_async_copy(basis_hbm.at[:, rows, :], basis_ref.at[:, rows, :], basis_sem.at[i])

    for i in range(4):
        chunk(i).start()

    def coords(d):
        return (d // sizes[1], lax.rem(d, sizes[1]))

    barrier = pltpu.get_barrier_semaphore()

    def greet(k, carry):
        pl.semaphore_signal(
            barrier, inc=1, device_id=coords(lax.rem(me + k, devices)), device_id_type=pl.DeviceIdType.MESH
        )
        return carry

    lax.fori_loop(1, devices, greet, 0)

    condense(
        elems, terms, coef_ref, basis_ref, lambda i: chunk(i).wait(), load_ref, shi_ref, slo_ref, diag_ref, lrow_ref,
        x_refs, d_ref, r_refs,
    )

    square = (LANES, LANES)
    sub = iota(square, 0)
    lane1 = iota((1, LANES), 1)

    def in_lanes(ref, fill):
        turned = jnp.concatenate([ref[...].astype(F32), jnp.zeros((6, LANES - elems), F32)], axis=1)
        out = jnp.full((1, LANES), fill, F32)
        for j in range(6):
            row = turned[j : j + 1]
            if j:
                row = pltpu.roll(row, 16 * j, 1)
            out = jnp.where(lane1 // 16 == j, row, out)
        return out

    def listed(first, second):
        out = jnp.zeros((1, LANES), jnp.int32)
        for at, (ref, base) in enumerate((first, second)):
            for i in range(2):
                for k in range(SHARED):
                    out = jnp.where(lane1 % 16 == 8 * at + SHARED * i + k, base + ref[0, i, k], out)
        return out

    own, far = (owned_ref, 0), (remote_ref, FACE_DEV)
    inc_t = jnp.where(sub.astype(F32) == in_lanes(face_ref, -1.0), 1.0, 0.0)
    inc = inc_t.T
    sel = jnp.where(sub == listed(own, far), 1.0, 0.0).astype(BF)
    place = jnp.where(sub == listed(far, own), 1.0, 0.0).T.astype(BF)
    inc_t = inc_t.astype(BF)
    inc = inc.astype(BF)
    inc_sel = jnp.dot(inc, sel, preferred_element_type=F32).astype(BF)
    out_mat = jnp.concatenate([inc, inc_sel], axis=1)
    perm = perm_ref[...]
    perm_t = permt_ref[...]
    code = in_lanes(code_ref, 0.0)
    lane32 = iota((32, LANES), 1)
    sub32 = iota((32, LANES), 0)
    in_group = lane32 // 16 == sub32 // 4
    lane4 = iota((4, LANES), 1)
    slot4 = lane4 % 16
    owned = lane32 < FACE_DEV

    def spread(field):
        a, b, c = split3(field)
        got = jnp.dot(jnp.concatenate([a, b, c], axis=0), inc_t, preferred_element_type=F32)
        pieces = []
        for s in range(3):
            part = got[32 * s : 32 * s + 32]
            pieces.append(
                jnp.concatenate([jnp.where(code == o, part, 0.0) for o in range(8)], axis=0).astype(BF)
            )
        return jnp.dot(perm, jnp.concatenate(pieces, axis=1), preferred_element_type=F32)

    def columns(values):
        blocks = []
        for j in range(6):
            block = jnp.zeros((32, LANES), F32)
            for s in range(3):
                part = values[:, LANES * s : LANES * s + LANES]
                shift = (16 * s - 16 * j) % LANES
                if shift:
                    part = pltpu.roll(part, shift, 1)
                block = jnp.where(lane32 // 16 == s, part, block)
            blocks.append(block)
        return jnp.concatenate(
            [blocks[0][3:25]] + [x[0:25] for x in blocks[1:]] + [jnp.zeros((106, LANES), F32), blocks[0][0:3]], axis=0
        ).astype(BF)

    def by_face(slices):
        out = jnp.zeros((32, LANES), F32)
        for j in range(6):
            part = jnp.concatenate([slices[j], jnp.zeros((7, LANES), F32)], axis=0)
            if j:
                part = pltpu.roll(part, 16 * j, 1)
            out = jnp.where(lane32 // 16 == j, part, out)
        return out

    def from_rows(t):
        return by_face([t[5 + 25 * j : 30 + 25 * j] for j in range(6)])

    def collect(values):
        turned = jnp.dot(perm_t, jnp.concatenate(split3(values), axis=1), preferred_element_type=F32)
        turned = turned[:, 0:128] + turned[:, 128:256] + turned[:, 256:384]
        placed = jnp.zeros((32, LANES), F32)
        for o in range(8):
            placed = jnp.where(code == o, turned[32 * o : 32 * o + 32], placed)
        both = jnp.dot(jnp.concatenate(split3(placed), axis=0), out_mat, preferred_element_type=F32)
        both = both[0:32] + both[32:64] + both[64:96]
        return both[:, 0:128], both[:, 128:256]

    def pack(message):
        kept = jnp.where(in_group, message, 0.0)
        out = kept[0:4]
        for g in range(1, 8):
            out = out + kept[4 * g : 4 * g + 4]
        return out

    def unpack(message):
        tall = jnp.where(in_group, jnp.concatenate([message] * 8, axis=0), 0.0)
        both = jnp.dot(jnp.concatenate(split3(tall), axis=0), place, preferred_element_type=F32)
        return both[0:32] + both[32:64] + both[64:96]

    def exchange(slot, parts):
        count = len(parts)
        buf_ref = buf_refs[slot]
        own_rows = send_ref.at[slot, 0 : 4 * count]
        for i, part in enumerate(parts):
            send_ref[slot, 4 * i : 4 * i + 4] = part
            buf_ref[me, 4 * i : 4 * i + 4] = part

        def send(first, second):
            pltpu.make_async_remote_copy(
                src_ref=own_rows,
                dst_ref=buf_ref.at[me],
                send_sem=send_sem.at[slot],
                recv_sem=recv_sem.at[slot],
                device_id=(
                    lax.rem(lax.axis_index(mesh_names[0]) + first, sizes[0]),
                    lax.rem(lax.axis_index(mesh_names[1]) + second, sizes[1]),
                ),
                device_id_type=pl.DeviceIdType.MESH,
            ).start()

        def send_at(k, carry):
            send(k // sizes[1], lax.rem(k, sizes[1]))
            return carry

        if devices > 64:
            lax.fori_loop(1, devices, send_at, 0)
        else:
            for second in sorted(range(sizes[1]), key=lambda k: -min(k, sizes[1] - k)):
                for first in reversed(range(sizes[0])):
                    if first or second:
                        send(first, second)
        every = buf_ref.at[pl.ds(0, devices - 1)]
        pltpu.make_async_copy(every, every, recv_sem.at[slot]).wait()
        pltpu.make_async_copy(every, every, send_sem.at[slot]).wait()
        from_upper = [buf_ref[upper_ref[0, i]] for i in range(2)]
        from_lower = [buf_ref[lower_ref[0, i]] for i in range(2)]
        out = []
        for i in range(count):
            rows = slice(4 * i, 4 * i + 4)
            mixed = jnp.where(
                slot4 < 4,
                from_upper[0][rows],
                jnp.where(
                    slot4 < 8, from_upper[1][rows], jnp.where(slot4 < 12, from_lower[0][rows], from_lower[1][rows])
                ),
            )
            out.append(unpack(mixed))
        return out

    spare = (lane4 // 16 == 6) & (iota((4, LANES), 0) == 1)

    diag_part, diag_out = collect(from_rows(diag_ref[...]))
    padded = jnp.concatenate([lrow_ref[...], jnp.zeros((LANES - elems, 256), F32)], axis=0)
    turned = jnp.concatenate([padded[:, 0:128].T, padded[:, 128:256].T], axis=0)
    slices = [jnp.concatenate([turned[253:256], turned[0:22]], axis=0)]
    slices += [turned[25 * j - 3 : 25 * j + 22] for j in range(1, 6)]
    load_part, load_out = collect(by_face(slices))
    pl.semaphore_wait(barrier, devices - 1)
    got = exchange(0, [pack(load_out), pack(diag_out)])
    live = (lane32 < FACE_DEV + REMOTE) & (sub32 < FACE_DOFS)
    residual = jnp.where(live, load_part + got[0], 0.0)
    weights = jnp.where(live, 1.0 / jnp.where(live, diag_part + got[1], 1.0), 0.0)

    trace = jnp.zeros((32, LANES), F32)
    direction = jnp.zeros((32, LANES), F32)
    image = jnp.zeros((32, LANES), F32)
    rz_now = None
    step = None
    row_lane = iota((ROWS, LANES), 1)
    row_elem = jnp.where(row_lane < 48, row_lane % 16, -1)
    for iteration in range(ITERS):
        precond = residual * weights
        values = spread(precond)
        cols = columns(values)
        total = jnp.zeros((ROWS, LANES), F32)
        for e in range(elems):
            rows = slice(ROWS * e, ROWS * e + ROWS)
            product = jnp.dot(shi_ref[rows], cols, preferred_element_type=F32)
            product = product + jnp.dot(slo_ref[rows], cols, preferred_element_type=F32)
            total = jnp.where(row_elem == e, product, total)
        total = total + pltpu.roll(total, LANES - 16, 1) + pltpu.roll(total, LANES - 32, 1)
        result = from_rows(total)
        flat = values[:, 0:128] + values[:, 128:256] + values[:, 256:384]
        curve_part = jnp.sum(jnp.where(lane32 < 6 * elems, flat * result, 0.0))
        rz_part = jnp.sum(jnp.where(owned, residual * precond, 0.0))
        part, out = collect(result)
        message = pack(out)
        message = jnp.where(spare, jnp.where(slot4 == 0, rz_part, jnp.where(slot4 == 1, curve_part, 0.0)), message)
        slot = iteration + 1
        got = exchange(slot, [message])[0]

        sums = jnp.sum(buf_refs[slot][...], axis=0)
        rz_next = jnp.sum(jnp.where(spare & (slot4 == 0), sums, 0.0), keepdims=True)
        curve = jnp.sum(jnp.where(spare & (slot4 == 1), sums, 0.0), keepdims=True)
        mapped = jnp.where(live, part + got, 0.0)
        if iteration == 0:
            step = rz_next / curve
            direction, image = precond, mapped
        else:
            ratio = rz_next / rz_now
            step = rz_next / (curve - ratio * rz_next / step)
            direction = precond + ratio * direction
            image = mapped + ratio * image
        rz_now = rz_next
        trace = trace + step * direction
        residual = residual - step * image
    out_ref[0] = trace
    out_ref[1] = residual


def on_device(
    sizes, basis_mats, coeffs, element_loads, elem_faces, orient_codes, shared_owned, shared_remote, lower_peers, upper_peers
):
    elems, terms = coeffs.shape
    vmem = pl.BlockSpec(memory_space=pltpu.VMEM)
    smem = pl.BlockSpec(memory_space=pltpu.SMEM)
    stack = permute_stack()
    devices = sizes[0] * sizes[1]
    result = pl.pallas_call(
        functools.partial(kernel, ("gx", "gy"), sizes, elems, terms),
        out_shape=jax.ShapeDtypeStruct((2, 32, LANES), F32),
        in_specs=[smem] * 5 + [pl.BlockSpec(memory_space=pltpu.HBM)] + [vmem] * 5,
        out_specs=vmem,
        scratch_shapes=[
            pltpu.VMEM((terms, LOCAL_DOFS, LOCAL_DOFS), F32),
            pltpu.VMEM((elems * ROWS, 256), BF),
            pltpu.VMEM((elems * ROWS, 256), BF),
            pltpu.VMEM((ROWS, LANES), F32),
            pltpu.VMEM((elems, 256), F32),
            [pltpu.VMEM((elems // WAYS, 288, 384), F32)] * WAYS,
            pltpu.VMEM((elems, NB, LANES), BF),
            [pltpu.VMEM((LANES, 384), BF)] * WAYS,
            [pltpu.VMEM((devices, 8 if i == 0 else 4, LANES), F32) for i in range(ITERS + 1)],
            pltpu.VMEM((ITERS + 1, 8, LANES), F32),
            pltpu.SemaphoreType.DMA((4,)),
            pltpu.SemaphoreType.DMA((ITERS + 1,)),
            pltpu.SemaphoreType.DMA((ITERS + 1,)),
        ],
        compiler_params=pltpu.CompilerParams(
            collective_id=0, has_side_effects=True, vmem_limit_bytes=56 * 1024 * 1024
        ),
        name="hdg",
    )(
        coeffs, upper_peers, lower_peers, shared_owned, shared_remote, basis_mats, element_loads, elem_faces.T, orient_codes.T,
        jnp.asarray(stack, BF), jnp.asarray(stack.T, BF),
    )
    return result[0, :FACE_DOFS, :FACE_DEV], result[1, :FACE_DOFS, :FACE_DEV]


def solution(mesh):
    row = P(("gx", "gy"), None)
    cube = P(("gx", "gy"), None, None)
    sizes = (mesh.shape["gx"], mesh.shape["gy"])
    return jax.shard_map(
        functools.partial(on_device, sizes),
        mesh=mesh,
        in_specs=(P(), row, row, row, row, cube, cube, row, row),
        out_specs=(P(None, ("gx", "gy")), P(None, ("gx", "gy"))),
        check_vma=False,
    )
```
